32 devices in a mesh: data: 4 (over y, z), dap: 8 (over x, core).
Axes of the slice: x: 4, y: 2, z: 2, core: 2. Of those that a mesh axis runs over, the one named last changes fastest.
The devices are a block of a 4x4x8 slice.
Arguments:
- msa_act: bfloat16 [1024, 64, 256], P(('data', 'dap')), parts along dimension 0
- pair_act: bfloat16 [256, 64, 128], P(('data', 'dap')), parts along dimension 0
- msa_mask: int32 [1024, 64], P('data'), parts along dimension 0
- res_mask: int32 [256], P('data'), parts along dimension 0
- w_row_bias: bfloat16 [2, 128, 8], replicated
- w_row_in: bfloat16 [2, 256, 4, 8, 32], replicated
- w_row_out: bfloat16 [2, 8, 32, 256], replicated
- w_col_in: bfloat16 [2, 256, 4, 8, 32], replicated
- w_col_out: bfloat16 [2, 8, 32, 256], replicated
- w_opm_in: bfloat16 [2, 256, 2, 32], replicated
- w_opm_out: bfloat16 [2, 32, 32, 128], replicated
- w_ts_bias: bfloat16 [2, 128, 4], replicated
- w_ts_in: bfloat16 [2, 128, 4, 4, 32], replicated
- w_ts_out: bfloat16 [2, 4, 32, 128], replicated
- w_te_bias: bfloat16 [2, 128, 4], replicated
- w_te_in: bfloat16 [2, 128, 4, 4, 32], replicated
- w_te_out: bfloat16 [2, 4, 32, 128], replicated
Outputs:
- output 1: bfloat16 [1024, 64, 256], P(('data', 'dap')), parts along dimension 0
- output 2: bfloat16 [256, 64, 128], P(('data', 'dap')), parts along dimension 0
There are 4 independent parts. The reference program is written for one: setup_inputs(seed, part) draws one part's arguments, and reference() takes and returns one part's arrays. A program takes and returns all parts, laid end to end along the dimension named above; an argument that names none is the same for every part.
All inputs are finite; a program needn't handle non-finite values.
Results may differ from the reference program's by a relative error of at most 0.0181275.
Values are sent between devices in bfloat16 or wider.
A program may use at most 768 MiB of HBM per device.

```python
import jax
import jax.numpy as jnp
from jax import lax

NR = 64
NS = 256
C_M = 256
C_Z = 128
HEADS_MSA = 8
HEAD_MSA = 32
HEADS_TRI = 4
HEAD_TRI = 32
OPM_DIM = 32


def draw_normal(key, shape, scale):
    return (jax.random.normal(key, shape, jnp.float32) * scale).astype(jnp.bfloat16)


def setup_inputs(seed: int = 0, part: int = 0) -> dict:
    base_key = jax.random.key(seed)
    part_keys = jax.random.split(jax.random.fold_in(base_key, part), 4)
    w_keys = jax.random.split(jax.random.fold_in(base_key, 1000), 13)
    width_msa = HEADS_MSA * HEAD_MSA
    width_tri = HEADS_TRI * HEAD_TRI
    return {
        'msa_act': draw_normal(part_keys[0], (NS, NR, C_M), 1.0),
        'pair_act': draw_normal(part_keys[1], (NR, NR, C_Z), 1.0),
        'msa_mask': (jax.random.randint(part_keys[2], (NS, NR), 0, 4) > 0).astype(jnp.int32),
        'res_mask': (jax.random.randint(part_keys[3], (NR,), 0, 4) > 0).astype(jnp.int32),
        'w_row_bias': draw_normal(w_keys[0], (2, C_Z, HEADS_MSA), 1.5 * C_Z ** -0.5),
        'w_row_in': draw_normal(w_keys[1], (2, C_M, 4, HEADS_MSA, HEAD_MSA), 1.25 * C_M ** -0.5),
        'w_row_out': draw_normal(w_keys[2], (2, HEADS_MSA, HEAD_MSA, C_M), 0.5 * width_msa ** -0.5),
        'w_col_in': draw_normal(w_keys[3], (2, C_M, 4, HEADS_MSA, HEAD_MSA), 1.25 * C_M ** -0.5),
        'w_col_out': draw_normal(w_keys[4], (2, HEADS_MSA, HEAD_MSA, C_M), 0.5 * width_msa ** -0.5),
        'w_opm_in': draw_normal(w_keys[5], (2, C_M, 2, OPM_DIM), C_M ** -0.5),
        'w_opm_out': draw_normal(w_keys[6], (2, OPM_DIM, OPM_DIM, C_Z), 0.25 * NS ** 0.5 / OPM_DIM),
        'w_ts_bias': draw_normal(w_keys[7], (2, C_Z, HEADS_TRI), 1.5 * C_Z ** -0.5),
        'w_ts_in': draw_normal(w_keys[8], (2, C_Z, 4, HEADS_TRI, HEAD_TRI), 1.25 * C_Z ** -0.5),
        'w_ts_out': draw_normal(w_keys[9], (2, HEADS_TRI, HEAD_TRI, C_Z), 0.5 * width_tri ** -0.5),
        'w_te_bias': draw_normal(w_keys[10], (2, C_Z, HEADS_TRI), 1.5 * C_Z ** -0.5),
        'w_te_in': draw_normal(w_keys[11], (2, C_Z, 4, HEADS_TRI, HEAD_TRI), 1.25 * C_Z ** -0.5),
        'w_te_out': draw_normal(w_keys[12], (2, HEADS_TRI, HEAD_TRI, C_Z), 0.5 * width_tri ** -0.5),
    }


def layer_norm(values):
    flat = values.astype(jnp.float32)
    row_mean = jnp.mean(flat, axis=-1, keepdims=True)
    centered = flat - row_mean
    row_var = jnp.mean(centered * centered, axis=-1, keepdims=True)
    return (centered * lax.rsqrt(row_var + 1e-5)).astype(jnp.bfloat16)


def add_residual(current, update):
    return (current.astype(jnp.float32) + update).astype(jnp.bfloat16)


def pair_bias(pair_ln, w_bias):
    num_res = pair_ln.shape[0]
    flat = jnp.dot(pair_ln.reshape(num_res * num_res, -1), w_bias, preferred_element_type=jnp.float32)
    return jnp.transpose(flat.astype(jnp.bfloat16).reshape(num_res, num_res, -1), (2, 0, 1))


def attend_one(x_ln, w_in, w_out, bias_hqk, key_mask):
    length = x_ln.shape[0]
    heads = w_in.shape[2]
    head_dim = w_in.shape[3]
    projected = jnp.dot(x_ln, w_in.reshape(w_in.shape[0], -1), preferred_element_type=jnp.float32)
    projected = projected.astype(jnp.bfloat16).astype(jnp.float32).reshape(length, 4, heads, head_dim)
    logits = jnp.einsum('qhd,khd->hqk', projected[:, 0], projected[:, 1]) * head_dim ** -0.5
    if bias_hqk is not None:
        logits = logits + bias_hqk.astype(jnp.float32)
    logits = jnp.where(key_mask[None, None, :] > 0, logits, -1e9)
    attn_probs = jax.nn.softmax(logits, axis=-1).astype(jnp.bfloat16).astype(jnp.float32)
    attended = jnp.einsum('hqk,khd->qhd', attn_probs, projected[:, 2])
    gated = (attended * jax.nn.sigmoid(projected[:, 3])).astype(jnp.bfloat16)
    return jnp.dot(gated.reshape(length, heads * head_dim), w_out.reshape(heads * head_dim, -1), preferred_element_type=jnp.float32)


def row_attention(msa_act, bias_hqk, msa_mask, w_in, w_out):
    def one_seq(inputs):
        seq_act, seq_mask = inputs
        return add_residual(seq_act, attend_one(layer_norm(seq_act), w_in, w_out, bias_hqk, seq_mask))
    return lax.map(one_seq, (msa_act, msa_mask))


def column_attention(msa_act, msa_mask, w_in, w_out):
    def one_col(inputs):
        col_act, col_mask = inputs
        return add_residual(col_act, attend_one(layer_norm(col_act), w_in, w_out, None, col_mask))
    result = lax.map(one_col, (jnp.swapaxes(msa_act, 0, 1), msa_mask.T))
    return jnp.swapaxes(result, 0, 1)


def outer_mean(msa_act, pair_act, msa_mask, w_in, w_out):
    num_seq, num_res, width = msa_act.shape
    mask_f32 = msa_mask.astype(jnp.float32)
    projected = jnp.dot(layer_norm(msa_act).reshape(num_seq * num_res, width), w_in.reshape(width, -1), preferred_element_type=jnp.float32)
    projected = projected.reshape(num_seq, num_res, 2, -1) * mask_f32[:, :, None, None]
    projected = projected.astype(jnp.bfloat16).astype(jnp.float32)
    left = jnp.swapaxes(projected[:, :, 0], 0, 1)
    right = projected[:, :, 1]
    pair_norm = jnp.dot(mask_f32.T, mask_f32)
    w_flat = w_out.reshape(-1, w_out.shape[-1])
    def one_row(inputs):
        left_row, norm_row = inputs
        outer = jnp.einsum('sp,sjq->jpq', left_row, right).astype(jnp.bfloat16)
        update = jnp.dot(outer.reshape(num_res, -1), w_flat, preferred_element_type=jnp.float32)
        return update / (1e-3 + norm_row[:, None])
    return add_residual(pair_act, lax.map(one_row, (left, pair_norm)))


def triangle_start(pair_act, res_mask, w_bias, w_in, w_out):
    pair_ln = layer_norm(pair_act)
    bias_hqk = pair_bias(pair_ln, w_bias)
    def one_row(row_ln):
        return attend_one(row_ln, w_in, w_out, bias_hqk, res_mask)
    return add_residual(pair_act, lax.map(one_row, pair_ln))


def triangle_end(pair_act, res_mask, w_bias, w_in, w_out):
    flipped = triangle_start(jnp.swapaxes(pair_act, 0, 1), res_mask, w_bias, w_in, w_out)
    return jnp.swapaxes(flipped, 0, 1)


def reference(msa_act, pair_act, msa_mask, res_mask, w_row_bias, w_row_in, w_row_out, w_col_in, w_col_out, w_opm_in, w_opm_out, w_ts_bias, w_ts_in, w_ts_out, w_te_bias, w_te_in, w_te_out):
    bias_first = pair_bias(layer_norm(pair_act), w_row_bias[0])
    msa_act = row_attention(msa_act, bias_first, msa_mask, w_row_in[0], w_row_out[0])
    msa_act = column_attention(msa_act, msa_mask, w_col_in[0], w_col_out[0])
    pair_act = outer_mean(msa_act, pair_act, msa_mask, w_opm_in[0], w_opm_out[0])
    pair_act = triangle_start(pair_act, res_mask, w_ts_bias[0], w_ts_in[0], w_ts_out[0])
    pair_act = triangle_end(pair_act, res_mask, w_te_bias[0], w_te_in[0], w_te_out[0])
    bias_second = pair_bias(layer_norm(pair_act), w_row_bias[1])
    msa_act = column_attention(msa_act, msa_mask, w_col_in[1], w_col_out[1])
    pair_act = outer_mean(msa_act, pair_act, msa_mask, w_opm_in[1], w_opm_out[1])
    msa_act = row_attention(msa_act, bias_second, msa_mask, w_row_in[1], w_row_out[1])
    pair_act = triangle_end(pair_act, res_mask, w_te_bias[1], w_te_in[1], w_te_out[1])
    pair_act = triangle_start(pair_act, res_mask, w_ts_bias[1], w_ts_in[1], w_ts_out[1])
    return msa_act, pair_act
```

```python
import functools
import math

import jax
import jax.numpy as jnp
from jax import lax
from jax.experimental import pallas as pl
from jax.experimental.pallas import tpu as pltpu
from jax.sharding import PartitionSpec as P

F32 = jnp.float32
BF16 = jnp.bfloat16
VMEM = pltpu.VMEM
HEAD = 32
RES = 2 * HEAD
LANE = 2 * RES
SEQ = 2 * LANE
WIDE = 4 * SEQ
OWN = 8
BLK = 16
LOG2E = math.log2(math.e)
NEG = -1e9 * LOG2E
SCALE = HEAD ** -0.5 * LOG2E


def dot_nn(a, b):
    return lax.dot_general(a, b, (((1,), (0,)), ((), ())), preferred_element_type=F32)


def dot_nt(a, b):
    return lax.dot_general(a, b, (((1,), (1,)), ((), ())), preferred_element_type=F32)


def dot_tn(a, b):
    return lax.dot_general(a, b, (((0,), (0,)), ((), ())), preferred_element_type=F32)


def iota(shape, axis):
    return lax.broadcasted_iota(jnp.int32, shape, axis)


def selector(rows, cols, source):
    return jnp.where(iota((rows, cols), 1) == source(iota((rows, cols), 0)), 1.0, 0.0).astype(BF16)


def rounded(x):
    return x.astype(BF16).astype(F32)


def layer_norm(x):
    scale = 1.0 / x.shape[-1]
    mean = jnp.sum(x, axis=-1, keepdims=True) * scale
    cen = x - mean
    var = jnp.sum(cen * cen, axis=-1, keepdims=True) * scale
    return (cen * lax.rsqrt(var + 1e-5)).astype(BF16)


def column(values, index):
    return jnp.sum(jnp.where(iota(values.shape, 1) == index, values, 0.0), axis=1, keepdims=True)


def softmax_rows(t):
    e = jnp.exp2(t - jnp.max(t, axis=0, keepdims=True))
    return (e * (1.0 / jnp.sum(e, axis=0, keepdims=True))).astype(BF16)


def interleave(*gens):
    gens = list(gens)
    while gens:
        for gen in list(gens):
            try:
                next(gen)
            except StopIteration:
                gens.remove(gen)


def project(load, w, bufs):
    q, k, v, g, _ = bufs
    hd = k.shape[1]
    x = layer_norm(load())
    yield
    q[...] = rounded(dot_nt(w[0:hd], x)).astype(q.dtype)
    yield
    k[...] = dot_nt(x, w[hd:2 * hd]).astype(BF16)
    yield
    v[...] = dot_nt(w[2 * hd:3 * hd], x).astype(BF16)
    yield
    g[...] = jax.nn.sigmoid(rounded(dot_nt(w[3 * hd:4 * hd], x)))
    yield


def col_attend(bufs, keep, ahead=2, late=1):
    q, k, v, g, o = bufs
    heads, length = q.shape[0] // HEAD, q.shape[1]
    per = LANE // HEAD

    def logits(h):
        r = h % per
        parts = [jnp.zeros((HEAD * r, length), BF16)] if r else []
        parts.append(q[h * HEAD:(h + 1) * HEAD, :])
        if r < per - 1:
            parts.append(jnp.zeros((HEAD * (per - 1 - r), length), BF16))
        lanes = slice(h // per * LANE, (h // per + 1) * LANE)
        return dot_nn(k[:, lanes], jnp.concatenate(parts, axis=0))

    pend = {i: logits(i) for i in range(ahead)}
    probs = {}
    for i in range(heads + late):
        if i + ahead < heads:
            pend[i + ahead] = logits(i + ahead)
        if i >= late:
            rows = slice((i - late) * HEAD, (i - late + 1) * HEAD)
            o[rows, :] = (dot_nn(v[rows, :], probs.pop(i - late)) * g[rows, :]).astype(BF16)
        if i < heads:
            probs[i] = softmax_rows(jnp.where(keep, pend.pop(i) * SCALE, NEG))
        yield


def row_attend(bufs, bias, masks, ahead=4, late=2):
    q, k, v, g, o = bufs
    groups = q.shape[0] // LANE
    low = iota((HEAD, LANE), 1) < RES
    zero = jnp.zeros((RES, LANE), BF16)

    def diag(a, b):
        return jnp.concatenate([jnp.concatenate([a, zero], axis=1), jnp.concatenate([zero, b], axis=1)], axis=0)

    def logits(pair, group, s):
        lanes = slice(pair * LANE, (pair + 1) * LANE)
        halves = []
        for t in range(2):
            h0 = group * LANE + t * RES
            even, odd = q[h0:h0 + HEAD, lanes], q[h0 + HEAD:h0 + RES, lanes]
            if s:
                even = pltpu.roll(even, RES, 1)
            else:
                odd = pltpu.roll(odd, RES, 1)
            halves.append(jnp.concatenate([jnp.where(low, even, 0.0), jnp.where(low, 0.0, odd)], axis=0).astype(BF16))
        r0 = (pair * 2 + s) * RES
        return dot_nn(k[r0:r0 + RES, group * LANE:(group + 1) * LANE], diag(*halves))

    def weighted(pair, group):
        lanes = slice(pair * LANE, (pair + 1) * LANE)
        first, second = probs.pop((pair, group, 0)), probs.pop((pair, group, 1))
        for t in range(2):
            part = slice(t * LANE, (t + 1) * LANE)
            rows = slice(group * LANE + t * RES, group * LANE + (t + 1) * RES)
            both = dot_nn(v[rows, lanes], diag(first[:, part], second[:, part]))
            b0, b1 = both[:, :LANE], both[:, LANE:]
            out = jnp.concatenate([jnp.where(low, b0[:HEAD], pltpu.roll(b1[:HEAD], RES, 1)),
                                   jnp.where(low, pltpu.roll(b0[HEAD:], RES, 1), b1[HEAD:])], axis=0)
            o[rows, lanes] = (out * g[rows, lanes]).astype(BF16)

    units = [(pair, group, s) for pair in range(2) for group in range(groups) for s in range(2)]
    pend = {u: logits(*u) for u in units[:ahead]}
    probs = {}
    for i in range(len(units) + late):
        if i + ahead < len(units):
            pend[units[i + ahead]] = logits(*units[i + ahead])
        if i >= late and units[i - late][2]:
            weighted(*units[i - late][:2])
        if i < len(units):
            pair, group, s = units[i]
            t = pend.pop(units[i]) * SCALE + bias[:, group * SEQ:(group + 1) * SEQ]
            probs[units[i]] = softmax_rows(jnp.where(masks[pair * 2 + s] > 0.5, t, NEG))
        yield


def kernel(n, m_ref, z_ref, mask_ref, res_ref,
           wrb_ref, wri_ref, wro_ref, wci_ref, wco_ref, woi_ref, woo_ref,
           wsb_ref, wsi_ref, wso_ref, web_ref, wei_ref, weo_ref,
           mo_ref, zo_ref,
           mf, zf, mcol, mrow, send_m, send_b, slot_b, bias_r, bias_t, mask_t, mask_n, rnorm, res_col,
           swap, rot, perm_s, perm_r, opm_rhs, opm_stage, opm_send, opm_all, opm_lhs, opm_w, opm_w4, opm_f, opm_t,
           send_z, slot_z,
           cq, ck, cv, cg, co, rq, rk, rv, rg, ro, tq, tk, tv, tg, to,
           ss_b, rs_b, ss_m, rs_m, ss_c, rs_c, ss_r, rs_r, ss_z, rs_z):
    me = lax.axis_index('dap')
    peers = [lax.rem(me + off, n) for off in range(1, n)]
    partner = me + 1 - 2 * lax.rem(me, 2)
    others = [lax.rem(me + off, n) for off in range(2, n, 2)]
    scope = jax.named_scope

    def remote(src, dst, send_sem, recv_sem, peer):
        return pltpu.make_async_remote_copy(src_ref=src, dst_ref=dst, send_sem=send_sem, recv_sem=recv_sem,
                                            device_id={'dap': peer}, device_id_type=pl.DeviceIdType.MESH)

    with scope('barrier'):
        barrier = pltpu.get_barrier_semaphore()
        for peer in peers:
            pl.semaphore_signal(barrier, inc=1, device_id={'dap': peer}, device_id_type=pl.DeviceIdType.MESH)
        pl.semaphore_wait(barrier, n - 1)

    def bias_send(idx, w_bias, heads):
        z_cat = jnp.concatenate([layer_norm(zf[l]) for l in range(OWN)], axis=1)
        w = w_bias.astype(F32)
        w_rows = jnp.concatenate([jnp.broadcast_to(w[h:h + 1], (OWN, LANE)) for h in range(heads)], axis=0)
        own = iota(w_rows.shape, 0) % OWN
        lhs = jnp.concatenate([jnp.where(own == l, w_rows, 0.0).astype(BF16) for l in range(OWN)], axis=1)
        part = dot_nt(lhs, jnp.concatenate([z_cat, z_cat], axis=0))
        if heads < OWN:
            part = jnp.concatenate([part, jnp.zeros((RES - part.shape[0], LANE), F32)], axis=0)
        part = part.astype(BF16)
        send_b[idx] = part
        slot_b[idx, me] = part
        for j, peer in enumerate(peers):
            remote(send_b.at[idx], slot_b.at[idx, me], ss_b.at[idx, j], rs_b.at[idx, me], peer).start()

    def bias_slots(idx):
        with scope('bias_wait'):
            for j, src in enumerate(peers):
                c = remote(send_b.at[idx], slot_b.at[idx, src], ss_b.at[idx, j], rs_b.at[idx, src], src)
                c.wait_send()
                c.wait_recv()
        return jnp.concatenate([slot_b[idx, d] for d in range(n)], axis=0)

    def bias_query_local(idx, heads, out):
        full = dot_tn(bias_slots(idx), swap[:, :heads * RES])
        out[...] = full[:RES] * LOG2E

    def bias_key_local(idx, out):
        full = dot_nn(swap[...], bias_slots(idx)) * LOG2E
        low = iota((RES, LANE), 1) < RES
        for t in range(OWN // 2):
            lanes = slice(t * LANE, (t + 1) * LANE)
            out[:, lanes] = jnp.where(low, full[lanes][:RES], full[lanes][RES:])

    row_bufs = lambda s: [buf.at[s] for buf in (rq, rk, rv, rg, ro)]

    def row_pass(b, load, store, first, count, hook):
        interleave(project(lambda: load(first), wri_ref.at[b], row_bufs(0)))
        ro[1] = jnp.zeros(ro.shape[1:], BF16)

        def finish(grp, slot, to):
            yield
            upd = dot_tn(ro[slot], wro_ref[b])
            yield
            store(to, rounded(load(grp) + upd).reshape(4, RES, SEQ))
            yield

        def body(step, carry):
            grp = first + step
            s = lax.rem(step, 2)
            masks = [column(mask_t[...], me * HEAD + grp * 4 + j) for j in range(4)]
            interleave(row_attend(row_bufs(s), bias_r, masks),
                       project(lambda: load(jnp.minimum(grp + 1, first + count - 1)), wri_ref.at[b], row_bufs(1 - s)),
                       finish(jnp.maximum(grp - 1, first), 1 - s, jnp.where(step == 0, OWN, grp - 1)))
            hook(step)
            return carry
        lax.fori_loop(0, count, body, 0)
        interleave(finish(first + count - 1, (count - 1) % 2, first + count - 1))

    def triangle(idx, w_in, w_out):
        bias_query_local(idx, 4, bias_t)
        with scope('tri'):
            masks = [res_col[:, 0:1]] * 4
            bufs = [[buf.at[c] for buf in (tq, tk, tv, tg, to)] for c in range(2)]
            load = [lambda c=c: zf[c * 4:(c + 1) * 4].reshape(SEQ, LANE) for c in range(2)]

            def finish(c):
                yield
                upd = dot_tn(to[c], w_out)
                yield
                zf[c * 4:(c + 1) * 4] = rounded(load[c]() + upd).reshape(4, RES, LANE)
            interleave(project(load[0], w_in, bufs[0]), project(load[1], w_in, bufs[1]))
            interleave(row_attend(bufs[0], bias_t, masks), row_attend(bufs[1], bias_t, masks))
            interleave(finish(0), finish(1))

    def z_send(idx):
        out = dot_nn(swap[...], zf[...].reshape(OWN * RES, LANE).astype(BF16)).astype(BF16)
        for d in range(n):
            send_z[idx, d] = out[d * RES:(d + 1) * RES]
        slot_z[idx, me] = send_z[idx, me]
        for j, peer in enumerate(peers):
            remote(send_z.at[idx, peer], slot_z.at[idx, me], ss_z.at[idx, j], rs_z.at[idx, me], peer).start()

    def z_recv(idx):
        with scope('z_wait'):
            for j, peer in enumerate(peers):
                c = remote(send_z.at[idx, peer], slot_z.at[idx, peer], ss_z.at[idx, j], rs_z.at[idx, peer], peer)
                c.wait_send()
                c.wait_recv()
        zf[...] = dot_nn(rot[...], jnp.concatenate([slot_z[idx, d] for d in range(n)], axis=0)).reshape(OWN, RES, LANE)

    def opm_start(b):
        out = dot_nn(selector(RES, RES, lambda r: r % OWN * OWN + r // OWN), opm_stage[0:RES].astype(BF16)).astype(BF16)
        opm_send[b] = out
        opm_all[b, me] = out
        for j, peer in enumerate([partner] + others):
            remote(opm_send.at[b], opm_all.at[b, me], ss_c.at[b, j], rs_c.at[b, me], peer).start()

    def opm_forward(b):
        with scope('opm_fwd'):
            for j, src in enumerate(others):
                remote(opm_all.at[b, src], opm_all.at[b, src], ss_c.at[b, len(others) + 1 + j], rs_c.at[b, src], partner).wait_recv()
                remote(opm_all.at[b, src], opm_all.at[b, src], ss_c.at[b, len(others) + 1 + j], rs_c.at[b, src], partner).start()

    def opm_finish(b, w_out):
        with scope('opm_wait'):
            for src in [partner] + [partner_of(o) for o in others]:
                remote(opm_send.at[b], opm_all.at[b, src], ss_c.at[b, 0], rs_c.at[b, src], partner).wait_recv()
            for j in range(n - 1):
                remote(opm_send.at[b], opm_all.at[b, me], ss_c.at[b, j], rs_c.at[b, me], partner).wait_send()
        with scope('opm'):
            lhs = opm_all[b].reshape(OWN * RES, WIDE)
            for pair in range(OWN // 2):
                part = rounded(dot_nn(lhs, opm_rhs[b, pair])).reshape(n, OWN, OWN, SEQ)
                for g in range(OWN):
                    rows = part[:, g].reshape(RES, SEQ)
                    for half in range(2):
                        l = pair * 2 + half
                        opm_lhs[l * RES:(l + 1) * RES, g * LANE:(g + 1) * LANE] = rows[:, half * LANE:(half + 1) * LANE]
            upd = dot_nn(opm_lhs[...].astype(BF16), w_out).reshape(OWN, RES, LANE)
            zf[...] = rounded(zf[...] + upd * rnorm[...])

    def partner_of(dev):
        return dev + 1 - 2 * lax.rem(dev, 2)

    zf[...] = z_ref[...].astype(F32)
    with scope('bias0'):
        bias_send(0, wrb_ref[0], OWN)

    with scope('consts'):
        flat = OWN * RES
        swap[...] = selector(flat, flat, lambda r: r // OWN % OWN * RES + r // RES * OWN + r % OWN)
        rot[...] = selector(flat, flat, lambda r: r // OWN % OWN * RES + r % OWN * OWN + r // RES)
        perm_s[...] = selector(LANE, LANE, lambda r: r % BLK * OWN + r // BLK)
        perm_r[...] = selector(SEQ, SEQ, lambda r: r % OWN * HEAD + r // OWN)
        m_t = mask_ref[...].astype(F32)
        mask_t[...] = m_t
        mask_n[...] = m_t.T
        norm = dot_nt(m_t.astype(BF16), m_t.astype(BF16))
        for l in range(OWN):
            rnorm[l] = jnp.broadcast_to(1.0 / (1e-3 + column(norm, me * OWN + l)), (RES, LANE))
        res = jnp.broadcast_to(res_ref[...].astype(F32), (RES, RES))
        eye = iota(res.shape, 0) == iota(res.shape, 1)
        res_col[...] = jnp.broadcast_to(jnp.sum(jnp.where(eye, res, 0.0), axis=1, keepdims=True), res_col.shape)
        spread = selector(HEAD, HEAD, lambda r: r % OWN * 4 + r // OWN)
        for b in range(2):
            a, c = woi_ref[b, 0:HEAD], woi_ref[b, HEAD:RES]
            gat, loc = (c, a) if b == 0 else (a, c)
            opm_w[b] = dot_nn(spread, gat).astype(BF16)
            opm_w4[b] = jnp.concatenate([loc] * 4, axis=0)
        opm_f[...] = woo_ref[0].astype(F32)
        for r in range(HEAD):
            opm_t[r * HEAD:(r + 1) * HEAD] = opm_f[pl.ds(r, HEAD, stride=HEAD), :].astype(BF16)
        co[1] = jnp.zeros(co.shape[1:], BF16)

    bias_query_local(0, OWN, bias_r)

    def send_chunk(chunk):
        rows = slice(chunk * BLK, (chunk + 1) * BLK)
        for off in range(n):
            dst = me if off == 0 else peers[off - 1]
            blk = mf[rows, pl.ds(pl.multiple_of(dst * OWN, OWN), OWN), :].reshape(LANE, SEQ).astype(BF16)
            blk = dot_nn(perm_s[...], blk).astype(BF16).reshape(OWN, BLK, SEQ)
            if off == 0:
                mcol[0:OWN, me * 2 + chunk] = blk
            else:
                send_m[chunk, off - 1] = blk
        for i in range(OWN):
            for j, peer in enumerate(peers):
                remote(send_m.at[chunk, j, i], mcol.at[i, me * 2 + chunk], ss_m.at[chunk], rs_m.at[chunk, i], peer).start()

    def load_first(grp):
        return m_ref[pl.ds(grp * 4, 4)].reshape(SEQ, SEQ).astype(F32)

    def store_first(grp, value):
        mf[pl.ds(grp * 4, 4)] = value

    for chunk in range(2):
        with scope('row1'):
            row_pass(0, load_first, store_first, chunk * 4, 4, lambda step: None)
        with scope('send_chunk'):
            send_chunk(chunk)

    col_bufs = lambda s: [buf.at[s] for buf in (cq, ck, cv, cg, co)]

    def residue_wait(i):
        for chunk in range(2):
            seven = send_m.at[chunk, :, 0]
            pltpu.make_async_copy(seven, seven, rs_m.at[chunk, i]).wait()

    def load_col(i):
        return mcol[i].reshape(SEQ, SEQ).astype(F32)

    def col_finish(b, i, slot):
        safe = jnp.minimum(i, OWN - 1)
        yield
        upd = dot_tn(co[slot], wco_ref[b])
        yield
        x = rounded(load_col(i) + upd)
        mcol[i] = x.astype(BF16).reshape(BLK, BLK, SEQ)
        x = layer_norm(x)
        yield
        local = (dot_nt(x, opm_w4[b]) * column(mask_n[...], me * OWN + safe)).astype(BF16)
        part = iota(local.shape, 1) // HEAD
        lanes = pl.ds(pl.multiple_of(lax.rem(i, 2) * LANE, LANE), LANE)
        for r in range(4):
            opm_rhs[b, lax.div(i, 2), r * SEQ:(r + 1) * SEQ, lanes] = jnp.where(part == r, local, jnp.zeros_like(local))
        yield
        gathered = rounded(dot_nt(opm_w[b], x) * mask_t[pl.ds(me * OWN + safe, 1), :])
        for r in range(4):
            opm_stage[pl.ds(pl.multiple_of(i * OWN, OWN), OWN), r * SEQ:(r + 1) * SEQ] = gathered[r * OWN:(r + 1) * OWN]
        yield

    def send_back(i):
        mrow[me, i] = mcol[i, pl.ds(me * 2, 2)]
        for j, peer in enumerate(peers):
            remote(mcol.at[i, pl.ds(peer * 2, 2)], mrow.at[me, i], ss_r.at[j], rs_r.at[me], peer).start()

    with scope('col_first'):
        residue_wait(0)
        interleave(project(lambda: load_col(0), wci_ref.at[0], col_bufs(0)))

    def at(step, when, fn):
        @pl.when(step == when)
        def _():
            fn()

    def stage_opm():
        opm_finish(0, opm_t[...])
        bias_send(1, wsb_ref[0], 4)

    def stage_start():
        triangle(1, wsi_ref.at[0], wso_ref[0])
        z_send(0)

    def stage_turn():
        z_recv(0)
        bias_send(2, web_ref[0], 4)

    def col_body(step, carry):
        @pl.when(step < OWN - 1)
        def _():
            residue_wait(step + 1)
        with scope('col'):
            s = lax.rem(step, 2)
            keep = column(mask_n[...], me * OWN + lax.rem(step, OWN)) > 0.5
            nxt, prev = step + 1, step - 1
            interleave(
                col_attend(col_bufs(s), keep),
                project(lambda: load_col(lax.rem(nxt, OWN)), wci_ref.at[jnp.minimum(lax.div(nxt, OWN), 1)], col_bufs(1 - s)),
                col_finish(jnp.where(prev >= OWN, 1, 0), jnp.where(step == 0, OWN, lax.rem(jnp.maximum(prev, 0), OWN)), 1 - s))

        @pl.when(prev >= OWN)
        def _():
            send_back(prev - OWN)
        at(step, OWN, lambda: opm_start(0))
        at(step, OWN + 2, lambda: opm_forward(0))
        at(step, OWN + 3, stage_opm)
        at(step, OWN + 5, stage_start)
        at(step, OWN + 7, stage_turn)
        return carry
    lax.fori_loop(0, 2 * OWN, col_body, 0)
    with scope('col_last'):
        interleave(col_finish(1, OWN - 1, 1))
        send_back(OWN - 1)

    triangle(2, wei_ref.at[0], weo_ref[0])
    with scope('bias3'):
        bias_send(3, wrb_ref[1], OWN)
        opm_start(1)

    with scope('m_wait'):
        for chunk in range(2):
            sent = send_m.at[chunk]
            pltpu.make_async_copy(sent, sent, ss_m.at[chunk]).wait()
        for j, src in enumerate(peers):
            pltpu.make_async_copy(mrow.at[src], mrow.at[src], rs_r.at[src]).wait()
            pltpu.make_async_copy(mrow.at[src], mrow.at[src], ss_r.at[j]).wait()
    with scope('m_perm'):
        for d in range(n):
            mf[0:HEAD, d * OWN:(d + 1) * OWN, :] = dot_nn(perm_r[...], mrow[d].reshape(SEQ, SEQ)).reshape(HEAD, OWN, SEQ)
    bias_key_local(3, bias_r)

    def stage_opm2():
        opm_finish(1, woo_ref[1])
        bias_send(4, web_ref[1], 4)

    def stage_end2():
        triangle(4, wei_ref.at[1], weo_ref[1])
        z_send(1)

    def stage_turn2():
        z_recv(1)
        bias_send(5, wsb_ref[1], 4)

    def row_hook(step):
        at(step, 2, lambda: opm_forward(1))
        at(step, 3, stage_opm2)
        at(step, 5, stage_end2)
        at(step, 7, stage_turn2)

    def load_second(grp):
        return mf[pl.ds(grp * 4, 4)].reshape(SEQ, SEQ)

    with scope('row2'):
        row_pass(1, load_second, store_first, 0, OWN, row_hook)
    triangle(5, wsi_ref.at[1], wso_ref[1])
    mo_ref[...] = mf[0:HEAD].astype(BF16)
    zo_ref[...] = zf[...].astype(BF16)


def solution(mesh):
    n = mesh.shape['dap']

    def local_step(msa, pair, msa_mask, res_mask, w_row_bias, w_row_in, w_row_out, w_col_in, w_col_out, w_opm_in, w_opm_out, w_ts_bias, w_ts_in, w_ts_out, w_te_bias, w_te_in, w_te_out):
        flat_in = lambda w: jnp.moveaxis(w, 1, -1).reshape(2, -1, w.shape[1])
        flat_out = lambda w: w.reshape(2, -1, w.shape[-1])
        args = (msa, pair, msa_mask.T, res_mask.reshape(1, -1),
                jnp.swapaxes(w_row_bias, 1, 2), flat_in(w_row_in), flat_out(w_row_out),
                flat_in(w_col_in), flat_out(w_col_out), flat_in(w_opm_in), flat_out(w_opm_out),
                jnp.swapaxes(w_ts_bias, 1, 2), flat_in(w_ts_in), flat_out(w_ts_out),
                jnp.swapaxes(w_te_bias, 1, 2), flat_in(w_te_in), flat_out(w_te_out))
        dma = pltpu.SemaphoreType.DMA

        def work_set(width, q_type):
            return [VMEM((2, width, SEQ), q_type), VMEM((2, SEQ, width), BF16), VMEM((2, width, SEQ), BF16),
                    VMEM((2, width, SEQ), F32), VMEM((2, width, SEQ), BF16)]
        flat = OWN * RES
        return pl.pallas_call(
            functools.partial(kernel, n),
            out_shape=(jax.ShapeDtypeStruct(msa.shape, BF16), jax.ShapeDtypeStruct(pair.shape, BF16)),
            in_specs=[pl.BlockSpec(memory_space=VMEM)] * len(args),
            out_specs=(pl.BlockSpec(memory_space=VMEM), pl.BlockSpec(memory_space=VMEM)),
            scratch_shapes=[
                VMEM((HEAD + 4, RES, SEQ), F32),
                VMEM((OWN, RES, LANE), F32),
                VMEM((OWN + 1, BLK, BLK, SEQ), BF16),
                VMEM((n, OWN, 2, BLK, SEQ), BF16),
                VMEM((2, n - 1, OWN, BLK, SEQ), BF16),
                VMEM((6, RES, LANE), BF16),
                VMEM((6, n, RES, LANE), BF16),
                VMEM((RES, flat), F32),
                VMEM((RES, SEQ), F32),
                VMEM((RES, SEQ), F32),
                VMEM((SEQ, RES), F32),
                VMEM((OWN, RES, LANE), F32),
                VMEM((RES, LANE), F32),
                VMEM((flat, flat), BF16),
                VMEM((flat, flat), BF16),
                VMEM((LANE, LANE), BF16),
                VMEM((SEQ, SEQ), BF16),
                VMEM((2, OWN // 2 + 1, WIDE, SEQ), BF16),
                VMEM((RES + OWN, WIDE), F32),
                VMEM((2, RES, WIDE), BF16),
                VMEM((2, n, RES, WIDE), BF16),
                VMEM((flat, WIDE), F32),
                VMEM((2, HEAD, SEQ), BF16),
                VMEM((2, LANE, SEQ), BF16),
                VMEM((WIDE, LANE), F32),
                VMEM((WIDE, LANE), BF16),
                VMEM((2, n, RES, LANE), BF16),
                VMEM((2, n, RES, LANE), BF16),
                *work_set(SEQ, BF16), *work_set(SEQ, F32), *work_set(LANE, F32),
                dma((6, n - 1)), dma((6, n)), dma((2,)), dma((2, OWN)), dma((2, n - 1)), dma((2, n)),
                dma((n - 1,)), dma((n,)), dma((2, n - 1)), dma((2, n)),
            ],
            compiler_params=pltpu.CompilerParams(
                collective_id=0, has_side_effects=True, vmem_limit_bytes=60 * WIDE * WIDE),
            name='evoformer',
        )(*args)

    in_specs = (P(('data', 'dap')), P(('data', 'dap')), P('data'), P('data')) + (P(),) * 13
    out_specs = (P(('data', 'dap')), P(('data', 'dap')))
    return jax.shard_map(local_step, mesh=mesh, in_specs=in_specs, out_specs=out_specs, check_vma=False)
```

```python
import functools
import math

import jax
import jax.numpy as jnp
from jax import lax
from jax.experimental import pallas as pl
from jax.experimental.pallas import tpu as pltpu
from jax.sharding import PartitionSpec as P

F32 = jnp.float32
BF16 = jnp.bfloat16
VMEM = pltpu.VMEM
HEAD = 32
RES = 2 * HEAD
LANE = 2 * RES
SEQ = 2 * LANE
WIDE = 4 * SEQ
OWN = 8
CHUNKS = 4
EARLY = 2
LOG2E = math.log2(math.e)
NEG = -1e9 * LOG2E
SCALE = HEAD ** -0.5 * LOG2E


def dot_nn(a, b):
    return lax.dot_general(a, b, (((1,), (0,)), ((), ())), preferred_element_type=F32)


def dot_nt(a, b):
    return lax.dot_general(a, b, (((1,), (1,)), ((), ())), preferred_element_type=F32)


def dot_tn(a, b):
    return lax.dot_general(a, b, (((0,), (0,)), ((), ())), preferred_element_type=F32)


def iota(shape, axis):
    return lax.broadcasted_iota(jnp.int32, shape, axis)


def selector(rows, cols, source):
    return jnp.where(iota((rows, cols), 1) == source(iota((rows, cols), 0)), 1.0, 0.0).astype(BF16)


def rounded(x):
    return x.astype(BF16).astype(F32)


def layer_norm(x):
    scale = 1.0 / x.shape[-1]
    mean = jnp.sum(x, axis=-1, keepdims=True) * scale
    cen = x - mean
    var = jnp.sum(cen * cen, axis=-1, keepdims=True) * scale
    return (cen * lax.rsqrt(var + 1e-5)).astype(BF16)


def column(values, index):
    return jnp.sum(jnp.where(iota(values.shape, 1) == index, values, 0.0), axis=1, keepdims=True)


def softmax_rows(t):
    e = jnp.exp2(t - jnp.max(t, axis=0, keepdims=True))
    return (e * (1.0 / jnp.sum(e, axis=0, keepdims=True))).astype(BF16)


def interleave(*gens):
    gens = list(gens)
    while gens:
        for gen in list(gens):
            try:
                next(gen)
            except StopIteration:
                gens.remove(gen)


def project(load, w, bufs):
    q, k, v, g, _ = bufs
    hd = k.shape[1]
    x = layer_norm(load())
    yield
    q[...] = rounded(dot_nt(w[0:hd], x)).astype(q.dtype)
    yield
    k[...] = dot_nt(x, w[hd:2 * hd]).astype(BF16)
    yield
    v[...] = dot_nt(w[2 * hd:3 * hd], x).astype(BF16)
    yield
    g[...] = jax.nn.sigmoid(rounded(dot_nt(w[3 * hd:4 * hd], x)))
    yield


def col_attend(bufs, keep, ahead=3, late=2):
    q, k, v, g, o = bufs
    heads, length = q.shape[0] // HEAD, q.shape[1]
    per = LANE // HEAD

    def logits(h):
        r = h % per
        parts = [jnp.zeros((HEAD * r, length), BF16)] if r else []
        parts.append(q[h * HEAD:(h + 1) * HEAD, :])
        if r < per - 1:
            parts.append(jnp.zeros((HEAD * (per - 1 - r), length), BF16))
        lanes = slice(h // per * LANE, (h // per + 1) * LANE)
        return dot_nn(k[:, lanes], jnp.concatenate(parts, axis=0))

    pend = {i: logits(i) for i in range(ahead)}
    probs = {}
    for i in range(heads + late):
        if i + ahead < heads:
            pend[i + ahead] = logits(i + ahead)
        if i >= late:
            rows = slice((i - late) * HEAD, (i - late + 1) * HEAD)
            o[rows, :] = (dot_nn(v[rows, :], probs.pop(i - late)) * g[rows, :]).astype(BF16)
        if i < heads:
            probs[i] = softmax_rows(jnp.where(keep, pend.pop(i) * SCALE, NEG))
        yield


def row_attend(bufs, bias, masks, ahead=4, late=2):
    q, k, v, g, o = bufs
    groups = q.shape[0] // LANE
    low = iota((HEAD, LANE), 1) < RES
    zero = jnp.zeros((RES, LANE), BF16)

    def diag(a, b):
        return jnp.concatenate([jnp.concatenate([a, zero], axis=1), jnp.concatenate([zero, b], axis=1)], axis=0)

    def logits(pair, group, s):
        lanes = slice(pair * LANE, (pair + 1) * LANE)
        halves = []
        for t in range(2):
            h0 = group * LANE + t * RES
            even, odd = q[h0:h0 + HEAD, lanes], q[h0 + HEAD:h0 + RES, lanes]
            if s:
                even = pltpu.roll(even, RES, 1)
            else:
                odd = pltpu.roll(odd, RES, 1)
            halves.append(jnp.concatenate([jnp.where(low, even, 0.0), jnp.where(low, 0.0, odd)], axis=0).astype(BF16))
        r0 = (pair * 2 + s) * RES
        return dot_nn(k[r0:r0 + RES, group * LANE:(group + 1) * LANE], diag(*halves))

    def weighted(pair, group):
        lanes = slice(pair * LANE, (pair + 1) * LANE)
        first, second = probs.pop((pair, group, 0)), probs.pop((pair, group, 1))
        for t in range(2):
            part = slice(t * LANE, (t + 1) * LANE)
            rows = slice(group * LANE + t * RES, group * LANE + (t + 1) * RES)
            both = dot_nn(v[rows, lanes], diag(first[:, part], second[:, part]))
            b0, b1 = both[:, :LANE], both[:, LANE:]
            out = jnp.concatenate([jnp.where(low, b0[:HEAD], pltpu.roll(b1[:HEAD], RES, 1)),
                                   jnp.where(low, pltpu.roll(b0[HEAD:], RES, 1), b1[HEAD:])], axis=0)
            o[rows, lanes] = (out * g[rows, lanes]).astype(BF16)

    units = [(pair, group, s) for pair in range(2) for group in range(groups) for s in range(2)]
    pend = {u: logits(*u) for u in units[:ahead]}
    probs = {}
    for i in range(len(units) + late):
        if i + ahead < len(units):
            pend[units[i + ahead]] = logits(*units[i + ahead])
        if i >= late and units[i - late][2]:
            weighted(*units[i - late][:2])
        if i < len(units):
            pair, group, s = units[i]
            t = pend.pop(units[i]) * SCALE + bias[:, group * SEQ:(group + 1) * SEQ]
            probs[units[i]] = softmax_rows(jnp.where(masks[pair * 2 + s] > 0.5, t, NEG))
        yield


def kernel(n, inputs, *refs):
    hbm, (mo_ref, zo_ref), held, sem_in = refs[:inputs], refs[inputs:inputs + 2], refs[inputs + 2:2 * inputs + 2], refs[2 * inputs + 2]
    body(n, hbm, sem_in, mo_ref, zo_ref, *held, *refs[2 * inputs + 3:])


def body(n, hbm, sem_in, mo_ref, zo_ref,
         m_ref, z_ref, mask_ref, res_ref,
         wrb_ref, wri_ref, wro_ref, wci_ref, wco_ref, woi_ref, woo_ref,
         wsb_ref, wsi_ref, wso_ref, web_ref, wei_ref, weo_ref,
         mf, zf, mcol, mrow, send_m, send_b, slot_b, bias_r, bias_t, mask_t, mask_n, rnorm, res_col,
           swap, rot, perm_s, perm_r, opm_rhs, opm_stage, opm_send, opm_all, opm_lhs, opm_w, opm_w4, opm_f, opm_t,
           send_z, slot_z,
           cq, ck, cv, cg, co, rq, rk, rv, rg, ro, tq, tk, tv, tg, to,
           ss_b, rs_b, ss_m, rs_m, rs_l, ss_c, rs_c, ss_r, rs_r, ss_z, rs_z):
    held = (m_ref, z_ref, mask_ref, res_ref, wrb_ref, wri_ref, wro_ref, wci_ref, wco_ref, woi_ref, woo_ref,
            wsb_ref, wsi_ref, wso_ref, web_ref, wei_ref, weo_ref)
    loads = [(dst, pltpu.make_async_copy(src, dst, sem_in.at[i])) for i, (src, dst) in enumerate(zip(hbm, held))]
    me = lax.axis_index('dap')
    peers = [lax.rem(me + off, n) for off in range(1, n)]
    partner = me + 1 - 2 * lax.rem(me, 2)
    others = [lax.rem(me + off, n) for off in (2, n - 2, 4)]
    scope = jax.named_scope

    def remote(src, dst, send_sem, recv_sem, peer):
        return pltpu.make_async_remote_copy(src_ref=src, dst_ref=dst, send_sem=send_sem, recv_sem=recv_sem,
                                            device_id={'dap': peer}, device_id_type=pl.DeviceIdType.MESH)

    def load_of(ref):
        return next(c for dst, c in loads if dst is ref)

    def need(*wanted):
        for ref in wanted:
            load_of(ref).wait()

    with scope('barrier'):
        barrier = pltpu.get_barrier_semaphore()
        for peer in peers:
            pl.semaphore_signal(barrier, inc=1, device_id={'dap': peer}, device_id_type=pl.DeviceIdType.MESH)
        order = (z_ref, wrb_ref, mask_ref, m_ref, wri_ref)
        for ref in order + tuple(ref for ref in held if not any(ref is o for o in order)):
            load_of(ref).start()

    def bias_part(idx, w_bias, heads):
        z_cat = jnp.concatenate([layer_norm(zf[l]) for l in range(OWN)], axis=1)
        w = w_bias.astype(F32)
        w_rows = jnp.concatenate([jnp.broadcast_to(w[h:h + 1], (OWN, LANE)) for h in range(heads)], axis=0)
        own = iota(w_rows.shape, 0) % OWN
        lhs = jnp.concatenate([jnp.where(own == l, w_rows, 0.0).astype(BF16) for l in range(OWN)], axis=1)
        part = dot_nt(lhs, jnp.concatenate([z_cat, z_cat], axis=0))
        if heads < OWN:
            part = jnp.concatenate([part, jnp.zeros((RES - part.shape[0], LANE), F32)], axis=0)
        part = part.astype(BF16)
        send_b[idx] = part
        slot_b[idx, me] = part

    def bias_send(idx, w_bias, heads):
        bias_part(idx, w_bias, heads)
        bias_start(idx)

    def bias_start(idx):
        for j, peer in enumerate(peers):
            remote(send_b.at[idx], slot_b.at[idx, me], ss_b.at[idx, j], rs_b.at[idx, me], peer).start()

    def bias_slots(idx):
        with scope('bias_wait'):
            for j, src in enumerate(peers):
                c = remote(send_b.at[idx], slot_b.at[idx, src], ss_b.at[idx, j], rs_b.at[idx, src], src)
                c.wait_send()
                c.wait_recv()
        return jnp.concatenate([slot_b[idx, d] for d in range(n)], axis=0)

    def bias_query_local(idx, heads, out):
        full = dot_tn(bias_slots(idx), swap[:, :heads * RES])
        out[...] = full[:RES] * LOG2E

    def bias_key_local(idx, heads, out):
        full = dot_nn(swap[:heads * RES, :], bias_slots(idx)) * LOG2E
        low = iota((RES, LANE), 1) < RES
        for t in range(heads // 2):
            lanes = slice(t * LANE, (t + 1) * LANE)
            out[:, lanes] = jnp.where(low, full[lanes][:RES], full[lanes][RES:])

    GROUPS = OWN

    def row_bufs(grp, slot):
        return [buf.at[grp] for buf in (rq, rk, rv, rg)] + [ro.at[slot]]

    def row_prepare(b, load):
        ro[2:4] = jnp.zeros((2, SEQ, SEQ), BF16)

        def body(half, carry):
            parts = []
            for j in range(GROUPS // 2):
                grp = half * (GROUPS // 2) + j
                parts.append(project(functools.partial(load, grp), wri_ref.at[b], row_bufs(grp, 0)))
            interleave(*parts)
            return carry
        lax.fori_loop(0, 2, body, 0)

    def row_pass(b, load, store, hook):
        def finish(grp, slot):
            yield
            upd = dot_tn(ro[slot], wro_ref[b])
            yield
            store(grp, rounded(load(grp) + upd).reshape(4, RES, SEQ))
            yield

        def body(step, carry):
            s = lax.rem(step, 2) * 2
            parts = []
            for j in range(2):
                grp = step * 2 + j
                masks = [column(mask_t[...], me * HEAD + grp * 4 + r) for r in range(4)]
                parts.append(row_attend(row_bufs(grp, s + j), bias_r, masks))
                parts.append(finish(jnp.maximum(grp - 2, 0), 2 - s + j))
            interleave(*parts)
            hook(step)
            return carry
        lax.fori_loop(0, GROUPS // 2, body, 0)
        interleave(finish(GROUPS - 2, 2), finish(GROUPS - 1, 3))

    def triangle(idx, w_in, w_out, assemble):
        assemble(idx, 4, bias_t)
        with scope('tri'):
            masks = [res_col[:, 0:1]] * 4
            bufs = [[buf.at[c] for buf in (tq, tk, tv, tg, to)] for c in range(2)]
            load = [lambda c=c: zf[c * 4:(c + 1) * 4].reshape(SEQ, LANE) for c in range(2)]

            def finish(c):
                yield
                upd = dot_tn(to[c], w_out)
                yield
                zf[c * 4:(c + 1) * 4] = rounded(load[c]() + upd).reshape(4, RES, LANE)
            interleave(project(load[0], w_in, bufs[0]), project(load[1], w_in, bufs[1]))
            interleave(row_attend(bufs[0], bias_t, masks), row_attend(bufs[1], bias_t, masks))
            interleave(finish(0), finish(1))

    def z_send(idx):
        out = dot_nn(swap[...], zf[...].reshape(OWN * RES, LANE).astype(BF16)).astype(BF16)
        for d in range(n):
            send_z[idx, d] = out[d * RES:(d + 1) * RES]
        slot_z[idx, me] = send_z[idx, me]
        for j, peer in enumerate(peers):
            remote(send_z.at[idx, peer], slot_z.at[idx, me], ss_z.at[idx, j], rs_z.at[idx, me], peer).start()

    def z_recv(idx):
        with scope('z_wait'):
            for j, peer in enumerate(peers):
                c = remote(send_z.at[idx, peer], slot_z.at[idx, peer], ss_z.at[idx, j], rs_z.at[idx, peer], peer)
                c.wait_send()
                c.wait_recv()
        zf[...] = dot_nn(rot[...], jnp.concatenate([slot_z[idx, d] for d in range(n)], axis=0)).reshape(OWN, RES, LANE)

    def partner_of(dev):
        return dev + 1 - 2 * lax.rem(dev, 2)

    def opm_start(b, half):
        turn = selector(HEAD, HEAD, lambda r: r % 4 * OWN + r // 4)
        out = dot_nn(turn, opm_stage[half * HEAD:(half + 1) * HEAD].astype(BF16)).astype(BF16)
        opm_send[b, half] = out
        opm_all[b, me, half] = out
        for j, peer in enumerate([partner] + others):
            remote(opm_send.at[b, half], opm_all.at[b, me, half], ss_c.at[b, half, j], rs_c.at[b, half, me], peer).start()

    def opm_forward(b, half):
        with scope('opm_fwd'):
            for j, src in enumerate(others):
                slot = opm_all.at[b, src, half]
                c = remote(slot, slot, ss_c.at[b, half, len(others) + 1 + j], rs_c.at[b, half, src], partner)
                c.wait_recv()
                c.start()

    def opm_finish(b, w_out):
        with scope('opm_wait'):
            for half in range(2):
                for src in [partner] + [partner_of(o) for o in others]:
                    slot = opm_all.at[b, src, half]
                    remote(slot, slot, ss_c.at[b, half, 0], rs_c.at[b, half, src], partner).wait_recv()
                for j in range(n - 1):
                    slot = opm_send.at[b, half]
                    remote(slot, slot, ss_c.at[b, half, j], rs_c.at[b, half, me], partner).wait_send()
        with scope('opm'):
            lhs = opm_all[b].reshape(OWN * RES, WIDE)
            first = iota((n * 4, OWN, SEQ), 1) < 4
            for pair in range(OWN // 2):
                part = rounded(dot_nn(lhs, opm_rhs[b, pair])).reshape(n, 2, 4, OWN, SEQ)
                h0, h1 = (part[:, half].reshape(n * 4, OWN, SEQ) for half in range(2))
                turned = (jnp.where(first, h0, pltpu.roll(h1, 4, 1)), jnp.where(first, pltpu.roll(h0, 4, 1), h1))
                for g in range(OWN):
                    rows = turned[g % 2].reshape(n, 4, OWN, SEQ)[:, g // 2].reshape(RES, SEQ)
                    for half in range(2):
                        l = pair * 2 + half
                        opm_lhs[l * RES:(l + 1) * RES, g * LANE:(g + 1) * LANE] = rows[:, half * LANE:(half + 1) * LANE]
            upd = dot_nn(opm_lhs[...].astype(BF16), w_out).reshape(OWN, RES, LANE)
            zf[...] = rounded(zf[...] + upd * rnorm[...])

    flat = OWN * RES
    with scope('bias0'):
        need(z_ref, wrb_ref)
        zf[...] = z_ref[...].astype(F32)
        bias_part(0, wrb_ref[0], OWN)
        swap[...] = selector(flat, flat, lambda r: r // OWN % OWN * RES + r // RES * OWN + r % OWN)
        perm_s[...] = selector(RES, RES, lambda r: r % OWN * OWN + r // OWN)
        pl.semaphore_wait(barrier, n - 1)
        bias_start(0)
        need(mask_ref)
        mask_t[...] = mask_ref[...].astype(F32)

    def constants():
        need(res_ref, woi_ref, woo_ref)
        rot[...] = selector(flat, flat, lambda r: r // OWN % OWN * RES + r % OWN * OWN + r // RES)
        perm_r[...] = selector(SEQ, SEQ, lambda r: r % OWN * HEAD + r // OWN)
        m_t = mask_t[...]
        mask_n[...] = m_t.T
        norm = dot_nt(m_t.astype(BF16), m_t.astype(BF16))
        for l in range(OWN):
            rnorm[l] = jnp.broadcast_to(1.0 / (1e-3 + column(norm, me * OWN + l)), (RES, LANE))
        res = jnp.broadcast_to(res_ref[...].astype(F32), (RES, RES))
        eye = iota(res.shape, 0) == iota(res.shape, 1)
        res_col[...] = jnp.broadcast_to(jnp.sum(jnp.where(eye, res, 0.0), axis=1, keepdims=True), res_col.shape)
        spread = selector(HEAD, HEAD, lambda r: r % OWN * 4 + r // OWN)
        for b in range(2):
            a, c = woi_ref[b, 0:HEAD], woi_ref[b, HEAD:RES]
            gat, loc = (c, a) if b == 0 else (a, c)
            opm_w[b] = dot_nn(spread, gat).astype(BF16)
            opm_w4[b] = jnp.concatenate([loc] * 4, axis=0)
        opm_f[...] = woo_ref[0].astype(F32)
        for r in range(HEAD):
            opm_t[r * HEAD:(r + 1) * HEAD] = opm_f[pl.ds(r, HEAD, stride=HEAD), :].astype(BF16)
        co[1] = jnp.zeros(co.shape[1:], BF16)

    def send_chunk(chunk):
        rows = pl.ds(pl.multiple_of(chunk * OWN, OWN), OWN)
        dests = [me] + peers
        blks = [mf[rows, pl.ds(pl.multiple_of(dst * OWN, OWN), OWN), :].reshape(RES, SEQ).astype(BF16) for dst in dests]
        out = dot_nn(perm_s[...], jnp.concatenate(blks, axis=1))
        mine = me * CHUNKS + chunk
        for j in range(n):
            blk = out[:, j * SEQ:(j + 1) * SEQ].reshape(OWN, OWN, SEQ).astype(BF16)
            if j == 0:
                mcol[0:OWN, mine] = blk
            else:
                send_m[chunk, j - 1] = blk
        for j, peer in enumerate(peers):
            remote(send_m.at[chunk, j, 0:EARLY], mcol.at[0:EARLY, mine], ss_m.at[0], rs_m.at[chunk], peer).start()

    def send_rest():
        for i in range(EARLY, OWN):
            for j, peer in enumerate(peers):
                remote(send_m.at[:, j, i], mcol.at[i, pl.ds(me * CHUNKS, CHUNKS)], ss_m.at[1], rs_l.at[i], peer).start()

    def at(step, when, fn):
        @pl.when(step == when)
        def _():
            fn()

    def load_first(grp):
        return m_ref[pl.ds(grp * 4, 4)].reshape(SEQ, SEQ).astype(F32)

    def store_first(grp, value):
        mf[pl.ds(grp * 4, 4)] = value

    with scope('prep1'):
        need(m_ref, wri_ref)
        row_prepare(0, load_first)
    bias_query_local(0, OWN, bias_r)
    with scope('row1'):
        need(wro_ref)
        def first_hook(step):
            @pl.when(step > 0)
            def _():
                send_chunk(step - 1)
        row_pass(0, load_first, store_first, first_hook)
    with scope('send_chunk'):
        send_chunk(CHUNKS - 1)
        send_rest()
    with scope('consts'):
        constants()

    col_bufs = lambda s: [buf.at[s] for buf in (cq, ck, cv, cg, co)]

    def residue_wait(i):
        slot = send_m.at[:, :, 0]
        pltpu.make_async_copy(slot, slot, rs_l.at[i]).wait()

    def load_col(i):
        return mcol[i].astype(F32).reshape(SEQ, SEQ)

    def col_finish(b, i, slot):
        safe = jnp.minimum(i, OWN - 1)
        yield
        upd = dot_tn(co[slot], wco_ref[b])
        yield
        x = rounded(load_col(i) + upd)
        mcol[i] = x.reshape(HEAD, OWN, SEQ).astype(BF16)
        x = layer_norm(x)
        yield
        local = (dot_nt(x, opm_w4[b]) * column(mask_n[...], me * OWN + safe)).astype(BF16)
        part = iota(local.shape, 1) // HEAD
        lanes = pl.ds(pl.multiple_of(lax.rem(i, 2) * LANE, LANE), LANE)
        for r in range(4):
            opm_rhs[b, lax.div(i, 2), r * SEQ:(r + 1) * SEQ, lanes] = jnp.where(part == r, local, jnp.zeros_like(local))
        yield
        gathered = rounded(dot_nt(opm_w[b], x) * mask_t[pl.ds(me * OWN + safe, 1), :])
        for r in range(4):
            opm_stage[pl.ds(pl.multiple_of(i * OWN, OWN), OWN), r * SEQ:(r + 1) * SEQ] = gathered[r * OWN:(r + 1) * OWN]
        yield

    def send_back(i):
        mrow[me, i] = mcol[i, pl.ds(me * CHUNKS, CHUNKS)]
        for j, peer in enumerate(peers):
            remote(mcol.at[i, pl.ds(peer * CHUNKS, CHUNKS)], mrow.at[me, i], ss_r.at[j], rs_r.at[me], peer).start()

    need(wsb_ref, wsi_ref, wso_ref, web_ref, wei_ref, weo_ref)
    with scope('col_first'):
        need(wci_ref, wco_ref)
        for chunk in range(CHUNKS):
            slot = send_m.at[chunk, :, 0:EARLY]
            pltpu.make_async_copy(slot, slot, rs_m.at[chunk]).wait()
        interleave(project(lambda: load_col(0), wci_ref.at[0], col_bufs(0)))

    def stage_opm():
        opm_forward(0, 1)
        opm_finish(0, opm_t[...])
        bias_send(1, wsb_ref[0], 4)

    def stage_start():
        triangle(1, wsi_ref.at[0], wso_ref[0], bias_query_local)
        z_send(0)
        bias_send(2, web_ref[0], 4)

    def stage_turn():
        z_recv(0)
        triangle(2, wei_ref.at[0], weo_ref[0], bias_key_local)
        bias_send(3, wrb_ref[1], OWN)

    def col_body(step, carry):
        @pl.when(jnp.logical_and(step >= EARLY - 1, step < OWN - 1))
        def _():
            residue_wait(step + 1)
        with scope('col'):
            s = lax.rem(step, 2)
            keep = column(mask_n[...], me * OWN + lax.rem(step, OWN)) > 0.5
            nxt, prev = step + 1, step - 1
            interleave(
                col_attend(col_bufs(s), keep),
                project(lambda: load_col(lax.rem(nxt, OWN)), wci_ref.at[jnp.minimum(lax.div(nxt, OWN), 1)], col_bufs(1 - s)),
                col_finish(jnp.where(prev >= OWN, 1, 0), jnp.where(step == 0, OWN, lax.rem(jnp.maximum(prev, 0), OWN)), 1 - s))

        at(step, 4, lambda: opm_start(0, 0))
        at(step, OWN, lambda: opm_start(0, 1))
        at(step, OWN, lambda: opm_forward(0, 0))
        at(step, OWN + 3, stage_opm)
        at(step, OWN + 4, lambda: opm_start(1, 0))
        at(step, OWN + 5, stage_start)
        at(step, OWN + 7, stage_turn)

        @pl.when(prev >= OWN)
        def _():
            send_back(prev - OWN)
        return carry
    lax.fori_loop(0, 2 * OWN, col_body, 0)
    with scope('col_last'):
        interleave(col_finish(1, OWN - 1, 1))
        opm_start(1, 1)
        send_back(OWN - 1)
    opm_forward(1, 0)

    opm_forward(1, 1)
    opm_finish(1, woo_ref[1])
    with scope('bias4'):
        bias_send(4, web_ref[1], 4)
    with scope('m_wait'):
        for half in range(2):
            sent = send_m.at[:, :, 0:EARLY] if half == 0 else send_m.at[:, :, EARLY:OWN]
            pltpu.make_async_copy(sent, sent, ss_m.at[half]).wait()
        for j, src in enumerate(peers):
            pltpu.make_async_copy(mrow.at[src], mrow.at[src], rs_r.at[src]).wait()
            pltpu.make_async_copy(mrow.at[src], mrow.at[src], ss_r.at[j]).wait()
    with scope('m_perm'):
        for d in range(n):
            mf[:, d * OWN:(d + 1) * OWN, :] = dot_nn(perm_r[...], mrow[d].astype(F32).reshape(SEQ, SEQ).astype(BF16)).reshape(HEAD, OWN, SEQ)

    def load_second(grp):
        return mf[pl.ds(grp * 4, 4)].reshape(SEQ, SEQ)

    def store_second(grp, value):
        mo_ref[pl.ds(grp * 4, 4)] = value.astype(BF16)

    with scope('prep2'):
        row_prepare(1, load_second)
    bias_key_local(3, OWN, bias_r)

    def stage_end2():
        triangle(4, wei_ref.at[1], weo_ref[1], bias_query_local)
        z_send(1)
        bias_send(5, wsb_ref[1], 4)

    with scope('row2'):
        row_pass(1, load_second, store_second, lambda step: at(step, 2, stage_end2))
    z_recv(1)
    triangle(5, wsi_ref.at[1], wso_ref[1], bias_key_local)
    zo_ref[...] = zf[...].astype(BF16)


def solution(mesh):
    n = mesh.shape['dap']

    def local_step(msa, pair, msa_mask, res_mask, w_row_bias, w_row_in, w_row_out, w_col_in, w_col_out, w_opm_in, w_opm_out, w_ts_bias, w_ts_in, w_ts_out, w_te_bias, w_te_in, w_te_out):
        flat_in = lambda w: jnp.moveaxis(w, 1, -1).reshape(2, -1, w.shape[1])
        flat_out = lambda w: w.reshape(2, -1, w.shape[-1])
        args = (msa, pair, msa_mask.T, res_mask.reshape(1, -1),
                jnp.swapaxes(w_row_bias, 1, 2), flat_in(w_row_in), flat_out(w_row_out),
                flat_in(w_col_in), flat_out(w_col_out), flat_in(w_opm_in), flat_out(w_opm_out),
                jnp.swapaxes(w_ts_bias, 1, 2), flat_in(w_ts_in), flat_out(w_ts_out),
                jnp.swapaxes(w_te_bias, 1, 2), flat_in(w_te_in), flat_out(w_te_out))
        dma = pltpu.SemaphoreType.DMA

        def work_set(slots, width, q_type, outs=2):
            return [VMEM((slots, width, SEQ), q_type), VMEM((slots, SEQ, width), BF16), VMEM((slots, width, SEQ), BF16),
                    VMEM((slots, width, SEQ), F32), VMEM((outs, width, SEQ), BF16)]
        flat = OWN * RES
        return pl.pallas_call(
            functools.partial(kernel, n, len(args)),
            out_shape=(jax.ShapeDtypeStruct(msa.shape, BF16), jax.ShapeDtypeStruct(pair.shape, BF16)),
            in_specs=[pl.BlockSpec(memory_space=pl.ANY)] * len(args),
            out_specs=(pl.BlockSpec(memory_space=VMEM), pl.BlockSpec(memory_space=VMEM)),
            scratch_shapes=[
                *[VMEM(a.shape, a.dtype) for a in args], dma((len(args),)),
                VMEM((HEAD, RES, SEQ), F32),
                VMEM((OWN, RES, LANE), F32),
                VMEM((OWN + 1, HEAD, OWN, SEQ), BF16),
                VMEM((n, OWN, CHUNKS, OWN, SEQ), BF16),
                VMEM((CHUNKS, n - 1, OWN, OWN, SEQ), BF16),
                VMEM((6, RES, LANE), BF16),
                VMEM((6, n, RES, LANE), BF16),
                VMEM((RES, flat), F32),
                VMEM((RES, SEQ), F32),
                VMEM((RES, SEQ), F32),
                VMEM((SEQ, RES), F32),
                VMEM((OWN, RES, LANE), F32),
                VMEM((RES, LANE), F32),
                VMEM((flat, flat), BF16),
                VMEM((flat, flat), BF16),
                VMEM((RES, RES), BF16),
                VMEM((SEQ, SEQ), BF16),
                VMEM((2, OWN // 2 + 1, WIDE, SEQ), BF16),
                VMEM((RES + OWN, WIDE), F32),
                VMEM((2, 2, HEAD, WIDE), BF16),
                VMEM((2, n, 2, HEAD, WIDE), BF16),
                VMEM((flat, WIDE), F32),
                VMEM((2, HEAD, SEQ), BF16),
                VMEM((2, LANE, SEQ), BF16),
                VMEM((WIDE, LANE), F32),
                VMEM((WIDE, LANE), BF16),
                VMEM((2, n, RES, LANE), BF16),
                VMEM((2, n, RES, LANE), BF16),
                *work_set(2, SEQ, BF16), *work_set(OWN, SEQ, F32, 4), *work_set(2, LANE, F32),
                dma((6, n - 1)), dma((6, n)), dma((2,)), dma((CHUNKS,)), dma((OWN,)), dma((2, 2, n - 1)), dma((2, 2, n)),
                dma((n - 1,)), dma((n,)), dma((2, n - 1)), dma((2, n)),
            ],
            compiler_params=pltpu.CompilerParams(
                collective_id=0, has_side_effects=True, vmem_limit_bytes=60 * WIDE * WIDE),
            name='evoformer',
        )(*args)

    in_specs = (P(('data', 'dap')), P(('data', 'dap')), P('data'), P('data')) + (P(),) * 13
    out_specs = (P(('data', 'dap')), P(('data', 'dap')))
    return jax.shard_map(local_step, mesh=mesh, in_specs=in_specs, out_specs=out_specs, check_vma=False)
```

```python
import functools
import math

import jax
import jax.numpy as jnp
from jax import lax
from jax.experimental import pallas as pl
from jax.experimental.pallas import tpu as pltpu
from jax.sharding import PartitionSpec as P

F32 = jnp.float32
BF16 = jnp.bfloat16
VMEM = pltpu.VMEM
HEAD = 32
RES = 2 * HEAD
LANE = 2 * RES
SEQ = 2 * LANE
WIDE = 4 * SEQ
OWN = 8
CHUNKS = 4
EARLY = 2
LOG2E = math.log2(math.e)
NEG = -1e9 * LOG2E
SCALE = HEAD ** -0.5 * LOG2E


def dot_nn(a, b):
    return lax.dot_general(a, b, (((1,), (0,)), ((), ())), preferred_element_type=F32)


def dot_nt(a, b):
    return lax.dot_general(a, b, (((1,), (1,)), ((), ())), preferred_element_type=F32)


def dot_tn(a, b):
    return lax.dot_general(a, b, (((0,), (0,)), ((), ())), preferred_element_type=F32)


def iota(shape, axis):
    return lax.broadcasted_iota(jnp.int32, shape, axis)


def selector(rows, cols, source):
    return jnp.where(iota((rows, cols), 1) == source(iota((rows, cols), 0)), 1.0, 0.0).astype(BF16)


def rounded(x):
    return x.astype(BF16).astype(F32)


def layer_norm(x):
    scale = 1.0 / x.shape[-1]
    mean = jnp.sum(x, axis=-1, keepdims=True) * scale
    cen = x - mean
    var = jnp.sum(cen * cen, axis=-1, keepdims=True) * scale
    return (cen * lax.rsqrt(var + 1e-5)).astype(BF16)


def column(values, index):
    return jnp.sum(jnp.where(iota(values.shape, 1) == index, values, 0.0), axis=1, keepdims=True)


def softmax_rows(t):
    e = jnp.exp2(t - jnp.max(t, axis=0, keepdims=True))
    return (e * (1.0 / jnp.sum(e, axis=0, keepdims=True))).astype(BF16)


def interleave(*gens):
    gens = list(gens)
    while gens:
        for gen in list(gens):
            try:
                next(gen)
            except StopIteration:
                gens.remove(gen)


def project(load, w, bufs):
    q, k, v, g, _ = bufs
    hd = k.shape[1]
    x = layer_norm(load())
    yield
    q[...] = rounded(dot_nt(w[0:hd], x)).astype(q.dtype)
    yield
    k[...] = dot_nt(x, w[hd:2 * hd]).astype(BF16)
    yield
    v[...] = dot_nt(w[2 * hd:3 * hd], x).astype(BF16)
    yield
    g[...] = jax.nn.sigmoid(rounded(dot_nt(w[3 * hd:4 * hd], x)))
    yield


def col_attend(bufs, keep, ahead=3, late=2):
    q, k, v, g, o = bufs
    heads, length = q.shape[0] // HEAD, q.shape[1]
    per = LANE // HEAD

    def logits(h):
        r = h % per
        parts = [jnp.zeros((HEAD * r, length), BF16)] if r else []
        parts.append(q[h * HEAD:(h + 1) * HEAD, :])
        if r < per - 1:
            parts.append(jnp.zeros((HEAD * (per - 1 - r), length), BF16))
        lanes = slice(h // per * LANE, (h // per + 1) * LANE)
        return dot_nn(k[:, lanes], jnp.concatenate(parts, axis=0))

    pend = {i: logits(i) for i in range(ahead)}
    probs = {}
    for i in range(heads + late):
        if i + ahead < heads:
            pend[i + ahead] = logits(i + ahead)
        if i >= late:
            rows = slice((i - late) * HEAD, (i - late + 1) * HEAD)
            o[rows, :] = (dot_nn(v[rows, :], probs.pop(i - late)) * g[rows, :]).astype(BF16)
        if i < heads:
            probs[i] = softmax_rows(jnp.where(keep, pend.pop(i) * SCALE, NEG))
        yield


def row_attend(bufs, bias, masks, ahead=4, late=2):
    q, k, v, g, o = bufs
    groups = q.shape[0] // LANE
    low = iota((HEAD, LANE), 1) < RES
    zero = jnp.zeros((RES, LANE), BF16)

    def diag(a, b):
        return jnp.concatenate([jnp.concatenate([a, zero], axis=1), jnp.concatenate([zero, b], axis=1)], axis=0)

    def logits(pair, group, s):
        lanes = slice(pair * LANE, (pair + 1) * LANE)
        halves = []
        for t in range(2):
            h0 = group * LANE + t * RES
            even, odd = q[h0:h0 + HEAD, lanes], q[h0 + HEAD:h0 + RES, lanes]
            if s:
                even = pltpu.roll(even, RES, 1)
            else:
                odd = pltpu.roll(odd, RES, 1)
            halves.append(jnp.concatenate([jnp.where(low, even, 0.0), jnp.where(low, 0.0, odd)], axis=0).astype(BF16))
        r0 = (pair * 2 + s) * RES
        return dot_nn(k[r0:r0 + RES, group * LANE:(group + 1) * LANE], diag(*halves))

    def weighted(pair, group):
        lanes = slice(pair * LANE, (pair + 1) * LANE)
        first, second = probs.pop((pair, group, 0)), probs.pop((pair, group, 1))
        for t in range(2):
            part = slice(t * LANE, (t + 1) * LANE)
            rows = slice(group * LANE + t * RES, group * LANE + (t + 1) * RES)
            both = dot_nn(v[rows, lanes], diag(first[:, part], second[:, part]))
            b0, b1 = both[:, :LANE], both[:, LANE:]
            out = jnp.concatenate([jnp.where(low, b0[:HEAD], pltpu.roll(b1[:HEAD], RES, 1)),
                                   jnp.where(low, pltpu.roll(b0[HEAD:], RES, 1), b1[HEAD:])], axis=0)
            o[rows, lanes] = (out * g[rows, lanes]).astype(BF16)

    units = [(pair, group, s) for pair in range(2) for group in range(groups) for s in range(2)]
    pend = {u: logits(*u) for u in units[:ahead]}
    probs = {}
    for i in range(len(units) + late):
        if i + ahead < len(units):
            pend[units[i + ahead]] = logits(*units[i + ahead])
        if i >= late and units[i - late][2]:
            weighted(*units[i - late][:2])
        if i < len(units):
            pair, group, s = units[i]
            t = pend.pop(units[i]) * SCALE + bias[:, group * SEQ:(group + 1) * SEQ]
            probs[units[i]] = softmax_rows(jnp.where(masks[pair * 2 + s] > 0.5, t, NEG))
        yield


def kernel(n, inputs, *refs):
    hbm, (mo_ref, zo_ref), held, sem_in = refs[:inputs], refs[inputs:inputs + 2], refs[inputs + 2:2 * inputs + 2], refs[2 * inputs + 2]
    body(n, hbm, sem_in, mo_ref, zo_ref, *held, *refs[2 * inputs + 3:])


def body(n, hbm, sem_in, mo_ref, zo_ref,
         m_ref, z_ref, mask_ref, res_ref,
         wrb_ref, wri_ref, wro_ref, wci_ref, wco_ref, woi_ref, woo_ref,
         wsb_ref, wsi_ref, wso_ref, web_ref, wei_ref, weo_ref,
         mf, zf, mcol, mrow, send_m, send_b, slot_b, bias_r, bias_t, mask_t, mask_n, rnorm, res_col,
           swap, rot, perm_s, perm_r, opm_rhs, opm_stage, opm_send, opm_all, opm_lhs, opm_w, opm_w4, opm_f, opm_t,
           send_z, slot_z,
           cq, ck, cv, cg, co, rq, rk, rv, rg, ro, tq, tk, tv, tg, to,
           ss_b, rs_b, ss_m, rs_m, rs_l, ss_c, rs_c, ss_r, rs_r, ss_z, rs_z):
    held = (m_ref, z_ref, mask_ref, res_ref, wrb_ref, wri_ref, wro_ref, wci_ref, wco_ref, woi_ref, woo_ref,
            wsb_ref, wsi_ref, wso_ref, web_ref, wei_ref, weo_ref)
    loads = [(dst, pltpu.make_async_copy(src, dst, sem_in.at[i])) for i, (src, dst) in enumerate(zip(hbm, held))]
    me = lax.axis_index('dap')
    peers = [lax.rem(me + off, n) for off in range(1, n)]
    partner = me + 1 - 2 * lax.rem(me, 2)
    others = [lax.rem(me + off, n) for off in (2, n - 2, 4)]
    scope = jax.named_scope

    def remote(src, dst, send_sem, recv_sem, peer):
        return pltpu.make_async_remote_copy(src_ref=src, dst_ref=dst, send_sem=send_sem, recv_sem=recv_sem,
                                            device_id={'dap': peer}, device_id_type=pl.DeviceIdType.MESH)

    def load_of(ref):
        return next(c for dst, c in loads if dst is ref)

    def need(*wanted):
        for ref in wanted:
            load_of(ref).wait()

    with scope('barrier'):
        barrier = pltpu.get_barrier_semaphore()
        for peer in peers:
            pl.semaphore_signal(barrier, inc=1, device_id={'dap': peer}, device_id_type=pl.DeviceIdType.MESH)
        order = (z_ref, wrb_ref, mask_ref, m_ref, wri_ref)
        for ref in order + tuple(ref for ref in held if not any(ref is o for o in order)):
            load_of(ref).start()

    def bias_part(idx, w_bias, heads):
        z_cat = jnp.concatenate([layer_norm(zf[l]) for l in range(OWN)], axis=1)
        w = w_bias.astype(F32)
        w_rows = jnp.concatenate([jnp.broadcast_to(w[h:h + 1], (OWN, LANE)) for h in range(heads)], axis=0)
        own = iota(w_rows.shape, 0) % OWN
        lhs = jnp.concatenate([jnp.where(own == l, w_rows, 0.0).astype(BF16) for l in range(OWN)], axis=1)
        part = dot_nt(lhs, jnp.concatenate([z_cat, z_cat], axis=0))
        if heads < OWN:
            part = jnp.concatenate([part, jnp.zeros((RES - part.shape[0], LANE), F32)], axis=0)
        part = part.astype(BF16)
        send_b[idx] = part
        slot_b[idx, me] = part

    def bias_send(idx, w_bias, heads):
        bias_part(idx, w_bias, heads)
        bias_start(idx)

    def bias_start(idx):
        for j, peer in enumerate(peers):
            remote(send_b.at[idx], slot_b.at[idx, me], ss_b.at[idx, j], rs_b.at[idx, me], peer).start()

    def bias_slots(idx):
        with scope('bias_wait'):
            for j, src in enumerate(peers):
                c = remote(send_b.at[idx], slot_b.at[idx, src], ss_b.at[idx, j], rs_b.at[idx, src], src)
                c.wait_send()
                c.wait_recv()
        return jnp.concatenate([slot_b[idx, d] for d in range(n)], axis=0)

    def bias_query_local(idx, heads, out):
        full = dot_tn(bias_slots(idx), swap[:, :heads * RES])
        out[...] = full[:RES] * LOG2E

    def bias_key_local(idx, heads, out):
        full = dot_nn(swap[:heads * RES, :], bias_slots(idx)) * LOG2E
        low = iota((RES, LANE), 1) < RES
        for t in range(heads // 2):
            lanes = slice(t * LANE, (t + 1) * LANE)
            out[:, lanes] = jnp.where(low, full[lanes][:RES], full[lanes][RES:])

    GROUPS = OWN

    def row_bufs(grp, slot):
        return [buf.at[grp] for buf in (rq, rk, rv, rg)] + [ro.at[slot]]

    def row_prepare(b, load):
        ro[2:4] = jnp.zeros((2, SEQ, SEQ), BF16)

        def body(half, carry):
            parts = []
            for j in range(GROUPS // 2):
                grp = half * (GROUPS // 2) + j
                parts.append(project(functools.partial(load, grp), wri_ref.at[b], row_bufs(grp, 0)))
            interleave(*parts)
            return carry
        lax.fori_loop(0, 2, body, 0)

    def row_pass(b, load, store, hook):
        def finish(grp, slot):
            yield
            upd = dot_tn(ro[slot], wro_ref[b])
            yield
            store(grp, rounded(load(grp) + upd).reshape(4, RES, SEQ))
            yield

        def body(step, carry):
            s = lax.rem(step, 2) * 2
            parts = []
            for j in range(2):
                grp = step * 2 + j
                masks = [column(mask_t[...], me * HEAD + grp * 4 + r) for r in range(4)]
                parts.append(row_attend(row_bufs(grp, s + j), bias_r, masks))
                parts.append(finish(jnp.maximum(grp - 2, 0), 2 - s + j))
            interleave(*parts)
            hook(step)
            return carry
        lax.fori_loop(0, GROUPS // 2, body, 0)
        interleave(finish(GROUPS - 2, 2), finish(GROUPS - 1, 3))

    def triangle(idx, w_in, w_out, assemble):
        assemble(idx, 4, bias_t)
        with scope('tri'):
            masks = [res_col[:, 0:1]] * 4
            bufs = [[buf.at[c] for buf in (tq, tk, tv, tg, to)] for c in range(2)]
            load = [lambda c=c: zf[c * 4:(c + 1) * 4].reshape(SEQ, LANE) for c in range(2)]

            def finish(c):
                yield
                upd = dot_tn(to[c], w_out)
                yield
                zf[c * 4:(c + 1) * 4] = rounded(load[c]() + upd).reshape(4, RES, LANE)
            interleave(project(load[0], w_in, bufs[0]), project(load[1], w_in, bufs[1]))
            interleave(row_attend(bufs[0], bias_t, masks), row_attend(bufs[1], bias_t, masks))
            interleave(finish(0), finish(1))

    def z_send(idx):
        out = dot_nn(swap[...], zf[...].reshape(OWN * RES, LANE).astype(BF16)).astype(BF16)
        for d in range(n):
            send_z[idx, d] = out[d * RES:(d + 1) * RES]
        slot_z[idx, me] = send_z[idx, me]
        for j, peer in enumerate(peers):
            remote(send_z.at[idx, peer], slot_z.at[idx, me], ss_z.at[idx, j], rs_z.at[idx, me], peer).start()

    def z_recv(idx):
        with scope('z_wait'):
            for j, peer in enumerate(peers):
                c = remote(send_z.at[idx, peer], slot_z.at[idx, peer], ss_z.at[idx, j], rs_z.at[idx, peer], peer)
                c.wait_send()
                c.wait_recv()
        zf[...] = dot_nn(rot[...], jnp.concatenate([slot_z[idx, d] for d in range(n)], axis=0)).reshape(OWN, RES, LANE)

    def partner_of(dev):
        return dev + 1 - 2 * lax.rem(dev, 2)

    def opm_start(b, half):
        turn = selector(HEAD, HEAD, lambda r: r % 4 * OWN + r // 4)
        out = dot_nn(turn, opm_stage[half * HEAD:(half + 1) * HEAD].astype(BF16)).astype(BF16)
        opm_send[b, half] = out
        opm_all[b, me, half] = out
        for j, peer in enumerate([partner] + others):
            remote(opm_send.at[b, half], opm_all.at[b, me, half], ss_c.at[b, half, j], rs_c.at[b, half, me], peer).start()

    def opm_forward(b, half):
        with scope('opm_fwd'):
            for j, src in enumerate(others):
                slot = opm_all.at[b, src, half]
                c = remote(slot, slot, ss_c.at[b, half, len(others) + 1 + j], rs_c.at[b, half, src], partner)
                c.wait_recv()
                c.start()

    def opm_finish(b, w_out):
        with scope('opm_wait'):
            for half in range(2):
                for src in [partner] + [partner_of(o) for o in others]:
                    slot = opm_all.at[b, src, half]
                    remote(slot, slot, ss_c.at[b, half, 0], rs_c.at[b, half, src], partner).wait_recv()
                for j in range(n - 1):
                    slot = opm_send.at[b, half]
                    remote(slot, slot, ss_c.at[b, half, j], rs_c.at[b, half, me], partner).wait_send()
        with scope('opm'):
            lhs = opm_all[b].reshape(OWN * RES, WIDE)
            first = iota((n * 4, OWN, SEQ), 1) < 4
            for pair in range(OWN // 2):
                part = rounded(dot_nn(lhs, opm_rhs[b, pair])).reshape(n, 2, 4, OWN, SEQ)
                h0, h1 = (part[:, half].reshape(n * 4, OWN, SEQ) for half in range(2))
                turned = (jnp.where(first, h0, pltpu.roll(h1, 4, 1)), jnp.where(first, pltpu.roll(h0, 4, 1), h1))
                for g in range(OWN):
                    rows = turned[g % 2].reshape(n, 4, OWN, SEQ)[:, g // 2].reshape(RES, SEQ)
                    for half in range(2):
                        l = pair * 2 + half
                        opm_lhs[l * RES:(l + 1) * RES, g * LANE:(g + 1) * LANE] = rows[:, half * LANE:(half + 1) * LANE]
            upd = dot_nn(opm_lhs[...].astype(BF16), w_out).reshape(OWN, RES, LANE)
            zf[...] = rounded(zf[...] + upd * rnorm[...])

    flat = OWN * RES
    with scope('bias0'):
        need(z_ref, wrb_ref)
        zf[...] = z_ref[...].astype(F32)
        bias_part(0, wrb_ref[0], OWN)
        swap[...] = selector(flat, flat, lambda r: r // OWN % OWN * RES + r // RES * OWN + r % OWN)
        perm_s[...] = selector(RES, RES, lambda r: r % OWN * OWN + r // OWN)
        pl.semaphore_wait(barrier, n - 1)
        bias_start(0)
        need(mask_ref)
        mask_t[...] = mask_ref[...].astype(F32)

    def constants():
        need(res_ref, woi_ref, woo_ref)
        rot[...] = selector(flat, flat, lambda r: r // OWN % OWN * RES + r % OWN * OWN + r // RES)
        perm_r[...] = selector(SEQ, SEQ, lambda r: r % OWN * HEAD + r // OWN)
        m_t = mask_t[...]
        mask_n[...] = m_t.T
        norm = dot_nt(m_t.astype(BF16), m_t.astype(BF16))
        for l in range(OWN):
            rnorm[l] = jnp.broadcast_to(1.0 / (1e-3 + column(norm, me * OWN + l)), (RES, LANE))
        res = jnp.broadcast_to(res_ref[...].astype(F32), (RES, RES))
        eye = iota(res.shape, 0) == iota(res.shape, 1)
        res_col[...] = jnp.broadcast_to(jnp.sum(jnp.where(eye, res, 0.0), axis=1, keepdims=True), res_col.shape)
        spread = selector(HEAD, HEAD, lambda r: r % OWN * 4 + r // OWN)
        for b in range(2):
            a, c = woi_ref[b, 0:HEAD], woi_ref[b, HEAD:RES]
            gat, loc = (c, a) if b == 0 else (a, c)
            opm_w[b] = dot_nn(spread, gat).astype(BF16)
            opm_w4[b] = jnp.concatenate([loc] * 4, axis=0)
        opm_f[...] = woo_ref[0].astype(F32)
        for r in range(HEAD):
            opm_t[r * HEAD:(r + 1) * HEAD] = opm_f[pl.ds(r, HEAD, stride=HEAD), :].astype(BF16)
        co[1] = jnp.zeros(co.shape[1:], BF16)

    def send_chunk(chunk):
        rows = pl.ds(pl.multiple_of(chunk * OWN, OWN), OWN)
        dests = [me] + peers
        blks = [mf[rows, pl.ds(pl.multiple_of(dst * OWN, OWN), OWN), :].reshape(RES, SEQ).astype(BF16) for dst in dests]
        out = dot_nn(perm_s[...], jnp.concatenate(blks, axis=1))
        mine = me * CHUNKS + chunk
        for j in range(n):
            blk = out[:, j * SEQ:(j + 1) * SEQ].reshape(OWN, OWN, SEQ).astype(BF16)
            if j == 0:
                mcol[0:OWN, mine] = blk
            else:
                send_m[chunk, j - 1] = blk
        for j, peer in enumerate(peers):
            remote(send_m.at[chunk, j, 0:EARLY], mcol.at[0:EARLY, mine], ss_m.at[0], rs_m.at[chunk], peer).start()

    def send_rest():
        for i in range(EARLY, OWN):
            for j, peer in enumerate(peers):
                remote(send_m.at[:, j, i], mcol.at[i, pl.ds(me * CHUNKS, CHUNKS)], ss_m.at[1], rs_l.at[i], peer).start()

    def at(step, when, fn):
        @pl.when(step == when)
        def _():
            fn()

    def load_first(grp):
        return m_ref[pl.ds(grp * 4, 4)].reshape(SEQ, SEQ).astype(F32)

    def store_first(grp, value):
        mf[pl.ds(grp * 4, 4)] = value

    with scope('prep1'):
        need(m_ref, wri_ref)
        row_prepare(0, load_first)
    bias_query_local(0, OWN, bias_r)
    with scope('row1'):
        need(wro_ref)
        def first_hook(step):
            @pl.when(step > 0)
            def _():
                send_chunk(step - 1)
        row_pass(0, load_first, store_first, first_hook)
    with scope('send_chunk'):
        send_chunk(CHUNKS - 1)
        send_rest()
    with scope('consts'):
        constants()

    col_bufs = lambda s: [buf.at[s] for buf in (cq, ck, cv, cg, co)]

    def residue_wait(i):
        slot = send_m.at[:, :, 0]
        pltpu.make_async_copy(slot, slot, rs_l.at[i]).wait()

    def load_col(i):
        return mcol[i].astype(F32).reshape(SEQ, SEQ)

    def col_finish(b, i, slot):
        safe = jnp.minimum(i, OWN - 1)
        yield
        upd = dot_tn(co[slot], wco_ref[b])
        yield
        x = rounded(load_col(i) + upd)
        mcol[i] = x.reshape(HEAD, OWN, SEQ).astype(BF16)
        x = layer_norm(x)
        yield
        local = (dot_nt(x, opm_w4[b]) * column(mask_n[...], me * OWN + safe)).astype(BF16)
        part = iota(local.shape, 1) // HEAD
        lanes = pl.ds(pl.multiple_of(lax.rem(i, 2) * LANE, LANE), LANE)
        for r in range(4):
            opm_rhs[b, lax.div(i, 2), r * SEQ:(r + 1) * SEQ, lanes] = jnp.where(part == r, local, jnp.zeros_like(local))
        yield
        gathered = rounded(dot_nt(opm_w[b], x) * mask_t[pl.ds(me * OWN + safe, 1), :])
        for r in range(4):
            opm_stage[pl.ds(pl.multiple_of(i * OWN, OWN), OWN), r * SEQ:(r + 1) * SEQ] = gathered[r * OWN:(r + 1) * OWN]
        yield

    def send_back(i):
        mrow[me, i] = mcol[i, pl.ds(me * CHUNKS, CHUNKS)]
        for j, peer in enumerate(peers):
            remote(mcol.at[i, pl.ds(peer * CHUNKS, CHUNKS)], mrow.at[me, i], ss_r.at[j], rs_r.at[me], peer).start()

    need(wsb_ref, wsi_ref, wso_ref, web_ref, wei_ref, weo_ref)
    with scope('col_first'):
        need(wci_ref, wco_ref)
        for chunk in range(CHUNKS):
            slot = send_m.at[chunk, :, 0:EARLY]
            pltpu.make_async_copy(slot, slot, rs_m.at[chunk]).wait()
        interleave(project(lambda: load_col(0), wci_ref.at[0], col_bufs(0)))

    def stage_opm():
        opm_forward(0, 1)
        opm_finish(0, opm_t[...])
        bias_send(1, wsb_ref[0], 4)

    def stage_start():
        triangle(1, wsi_ref.at[0], wso_ref[0], bias_query_local)
        z_send(0)
        bias_send(2, web_ref[0], 4)

    def col_body(step, carry):
        @pl.when(jnp.logical_and(step >= EARLY - 1, step < OWN - 1))
        def _():
            residue_wait(step + 1)
        with scope('col'):
            s = lax.rem(step, 2)
            keep = column(mask_n[...], me * OWN + lax.rem(step, OWN)) > 0.5
            nxt, prev = step + 1, step - 1
            interleave(
                col_attend(col_bufs(s), keep),
                project(lambda: load_col(lax.rem(nxt, OWN)), wci_ref.at[jnp.minimum(lax.div(nxt, OWN), 1)], col_bufs(1 - s)),
                col_finish(jnp.where(prev >= OWN, 1, 0), jnp.where(step == 0, OWN, lax.rem(jnp.maximum(prev, 0), OWN)), 1 - s))

        at(step, 4, lambda: opm_start(0, 0))
        at(step, OWN, lambda: opm_start(0, 1))
        at(step, OWN, lambda: opm_forward(0, 0))
        at(step, OWN + 4, stage_opm)
        at(step, OWN + 4, lambda: opm_start(1, 0))
        at(step, OWN + 6, stage_start)

        @pl.when(prev >= OWN)
        def _():
            send_back(prev - OWN)
        return carry
    lax.fori_loop(0, 2 * OWN, col_body, 0)
    with scope('col_last'):
        interleave(col_finish(1, OWN - 1, 1))
        send_back(OWN - 1)
        opm_start(1, 1)

    z_recv(0)
    triangle(2, wei_ref.at[0], weo_ref[0], bias_key_local)

    with scope('bias3'):
        bias_send(3, wrb_ref[1], OWN)
    opm_forward(1, 0)
    with scope('m_wait'):
        for half in range(2):
            sent = send_m.at[:, :, 0:EARLY] if half == 0 else send_m.at[:, :, EARLY:OWN]
            pltpu.make_async_copy(sent, sent, ss_m.at[half]).wait()
        for j, src in enumerate(peers):
            pltpu.make_async_copy(mrow.at[src], mrow.at[src], rs_r.at[src]).wait()
            pltpu.make_async_copy(mrow.at[src], mrow.at[src], ss_r.at[j]).wait()
    with scope('m_perm'):
        for d in range(n):
            mf[:, d * OWN:(d + 1) * OWN, :] = dot_nn(perm_r[...], mrow[d].astype(F32).reshape(SEQ, SEQ).astype(BF16)).reshape(HEAD, OWN, SEQ)

    def load_second(grp):
        return mf[pl.ds(grp * 4, 4)].reshape(SEQ, SEQ)

    def store_second(grp, value):
        mo_ref[pl.ds(grp * 4, 4)] = value.astype(BF16)

    with scope('prep2'):
        row_prepare(1, load_second)
    opm_forward(1, 1)
    opm_finish(1, woo_ref[1])
    with scope('bias4'):
        bias_send(4, web_ref[1], 4)
    bias_key_local(3, OWN, bias_r)

    def stage_end2():
        triangle(4, wei_ref.at[1], weo_ref[1], bias_query_local)
        z_send(1)
        bias_send(5, wsb_ref[1], 4)

    with scope('row2'):
        row_pass(1, load_second, store_second, lambda step: at(step, 2, stage_end2))
    z_recv(1)
    triangle(5, wsi_ref.at[1], wso_ref[1], bias_key_local)
    zo_ref[...] = zf[...].astype(BF16)


def solution(mesh):
    n = mesh.shape['dap']

    def local_step(msa, pair, msa_mask, res_mask, w_row_bias, w_row_in, w_row_out, w_col_in, w_col_out, w_opm_in, w_opm_out, w_ts_bias, w_ts_in, w_ts_out, w_te_bias, w_te_in, w_te_out):
        flat_in = lambda w: jnp.moveaxis(w, 1, -1).reshape(2, -1, w.shape[1])
        flat_out = lambda w: w.reshape(2, -1, w.shape[-1])
        args = (msa, pair, msa_mask.T, res_mask.reshape(1, -1),
                jnp.swapaxes(w_row_bias, 1, 2), flat_in(w_row_in), flat_out(w_row_out),
                flat_in(w_col_in), flat_out(w_col_out), flat_in(w_opm_in), flat_out(w_opm_out),
                jnp.swapaxes(w_ts_bias, 1, 2), flat_in(w_ts_in), flat_out(w_ts_out),
                jnp.swapaxes(w_te_bias, 1, 2), flat_in(w_te_in), flat_out(w_te_out))
        dma = pltpu.SemaphoreType.DMA

        def work_set(slots, width, q_type, outs=2):
            return [VMEM((slots, width, SEQ), q_type), VMEM((slots, SEQ, width), BF16), VMEM((slots, width, SEQ), BF16),
                    VMEM((slots, width, SEQ), F32), VMEM((outs, width, SEQ), BF16)]
        flat = OWN * RES
        return pl.pallas_call(
            functools.partial(kernel, n, len(args)),
            out_shape=(jax.ShapeDtypeStruct(msa.shape, BF16), jax.ShapeDtypeStruct(pair.shape, BF16)),
            in_specs=[pl.BlockSpec(memory_space=pl.ANY)] * len(args),
            out_specs=(pl.BlockSpec(memory_space=VMEM), pl.BlockSpec(memory_space=VMEM)),
            scratch_shapes=[
                *[VMEM(a.shape, a.dtype) for a in args], dma((len(args),)),
                VMEM((HEAD, RES, SEQ), F32),
                VMEM((OWN, RES, LANE), F32),
                VMEM((OWN + 1, HEAD, OWN, SEQ), BF16),
                VMEM((n, OWN, CHUNKS, OWN, SEQ), BF16),
                VMEM((CHUNKS, n - 1, OWN, OWN, SEQ), BF16),
                VMEM((6, RES, LANE), BF16),
                VMEM((6, n, RES, LANE), BF16),
                VMEM((RES, flat), F32),
                VMEM((RES, SEQ), F32),
                VMEM((RES, SEQ), F32),
                VMEM((SEQ, RES), F32),
                VMEM((OWN, RES, LANE), F32),
                VMEM((RES, LANE), F32),
                VMEM((flat, flat), BF16),
                VMEM((flat, flat), BF16),
                VMEM((RES, RES), BF16),
                VMEM((SEQ, SEQ), BF16),
                VMEM((2, OWN // 2 + 1, WIDE, SEQ), BF16),
                VMEM((RES + OWN, WIDE), F32),
                VMEM((2, 2, HEAD, WIDE), BF16),
                VMEM((2, n, 2, HEAD, WIDE), BF16),
                VMEM((flat, WIDE), F32),
                VMEM((2, HEAD, SEQ), BF16),
                VMEM((2, LANE, SEQ), BF16),
                VMEM((WIDE, LANE), F32),
                VMEM((WIDE, LANE), BF16),
                VMEM((2, n, RES, LANE), BF16),
                VMEM((2, n, RES, LANE), BF16),
                *work_set(2, SEQ, BF16), *work_set(OWN, SEQ, F32, 4), *work_set(2, LANE, F32),
                dma((6, n - 1)), dma((6, n)), dma((2,)), dma((CHUNKS,)), dma((OWN,)), dma((2, 2, n - 1)), dma((2, 2, n)),
                dma((n - 1,)), dma((n,)), dma((2, n - 1)), dma((2, n)),
            ],
            compiler_params=pltpu.CompilerParams(
                collective_id=0, has_side_effects=True, vmem_limit_bytes=60 * WIDE * WIDE),
            name='evoformer',
        )(*args)

    in_specs = (P(('data', 'dap')), P(('data', 'dap')), P('data'), P('data')) + (P(),) * 13
    out_specs = (P(('data', 'dap')), P(('data', 'dap')))
    return jax.shard_map(local_step, mesh=mesh, in_specs=in_specs, out_specs=out_specs, check_vma=False)
```

```python
import functools
import math

import jax
import jax.numpy as jnp
from jax import lax
from jax.experimental import pallas as pl
from jax.experimental.pallas import tpu as pltpu
from jax.sharding import PartitionSpec as P

F32 = jnp.float32
BF16 = jnp.bfloat16
VMEM = pltpu.VMEM
HEAD = 32
RES = 2 * HEAD
LANE = 2 * RES
SEQ = 2 * LANE
WIDE = 4 * SEQ
OWN = 8
CHUNKS = 4
EARLY = 2
LOG2E = math.log2(math.e)
NEG = -1e9 * LOG2E
SCALE = HEAD ** -0.5 * LOG2E


def dot_nn(a, b):
    return lax.dot_general(a, b, (((1,), (0,)), ((), ())), preferred_element_type=F32)


def dot_nt(a, b):
    return lax.dot_general(a, b, (((1,), (1,)), ((), ())), preferred_element_type=F32)


def dot_tn(a, b):
    return lax.dot_general(a, b, (((0,), (0,)), ((), ())), preferred_element_type=F32)


def iota(shape, axis):
    return lax.broadcasted_iota(jnp.int32, shape, axis)


def selector(rows, cols, source):
    return jnp.where(iota((rows, cols), 1) == source(iota((rows, cols), 0)), 1.0, 0.0).astype(BF16)


def rounded(x):
    return x.astype(BF16).astype(F32)


def layer_norm(x):
    scale = 1.0 / x.shape[-1]
    mean = jnp.sum(x, axis=-1, keepdims=True) * scale
    cen = x - mean
    var = jnp.sum(cen * cen, axis=-1, keepdims=True) * scale
    return (cen * lax.rsqrt(var + 1e-5)).astype(BF16)


def column(values, index):
    return jnp.sum(jnp.where(iota(values.shape, 1) == index, values, 0.0), axis=1, keepdims=True)


def softmax_rows(t):
    e = jnp.exp2(t - jnp.max(t, axis=0, keepdims=True))
    return (e * (1.0 / jnp.sum(e, axis=0, keepdims=True))).astype(BF16)


def interleave(*gens):
    gens = list(gens)
    while gens:
        for gen in list(gens):
            try:
                next(gen)
            except StopIteration:
                gens.remove(gen)


def project(load, w, bufs):
    q, k, v, g, _ = bufs
    hd = k.shape[1]
    x = layer_norm(load())
    yield
    q[...] = rounded(dot_nt(w[0:hd], x)).astype(q.dtype)
    yield
    k[...] = dot_nt(x, w[hd:2 * hd]).astype(BF16)
    yield
    v[...] = dot_nt(w[2 * hd:3 * hd], x).astype(BF16)
    yield
    g[...] = jax.nn.sigmoid(rounded(dot_nt(w[3 * hd:4 * hd], x)))
    yield


def col_attend(bufs, keep, ahead=4, late=2):
    q, k, v, g, o = bufs
    heads, length = q.shape[0] // HEAD, q.shape[1]
    per = LANE // HEAD

    def logits(h):
        r = h % per
        parts = [jnp.zeros((HEAD * r, length), BF16)] if r else []
        parts.append(q[h * HEAD:(h + 1) * HEAD, :])
        if r < per - 1:
            parts.append(jnp.zeros((HEAD * (per - 1 - r), length), BF16))
        lanes = slice(h // per * LANE, (h // per + 1) * LANE)
        return dot_nn(k[:, lanes], jnp.concatenate(parts, axis=0))

    pend = {i: logits(i) for i in range(ahead)}
    probs = {}
    for i in range(heads + late):
        if i + ahead < heads:
            pend[i + ahead] = logits(i + ahead)
        if i >= late:
            rows = slice((i - late) * HEAD, (i - late + 1) * HEAD)
            o[rows, :] = (dot_nn(v[rows, :], probs.pop(i - late)) * g[rows, :]).astype(BF16)
        if i < heads:
            probs[i] = softmax_rows(jnp.where(keep, pend.pop(i) * SCALE, NEG))
        yield


def row_attend(bufs, bias, masks, ahead=4, late=2):
    q, k, v, g, o = bufs
    groups = q.shape[0] // LANE
    low = iota((HEAD, LANE), 1) < RES
    zero = jnp.zeros((RES, LANE), BF16)

    def diag(a, b):
        return jnp.concatenate([jnp.concatenate([a, zero], axis=1), jnp.concatenate([zero, b], axis=1)], axis=0)

    def logits(pair, group, s):
        lanes = slice(pair * LANE, (pair + 1) * LANE)
        halves = []
        for t in range(2):
            h0 = group * LANE + t * RES
            even, odd = q[h0:h0 + HEAD, lanes], q[h0 + HEAD:h0 + RES, lanes]
            if s:
                even = pltpu.roll(even, RES, 1)
            else:
                odd = pltpu.roll(odd, RES, 1)
            halves.append(jnp.concatenate([jnp.where(low, even, 0.0), jnp.where(low, 0.0, odd)], axis=0).astype(BF16))
        r0 = (pair * 2 + s) * RES
        return dot_nn(k[r0:r0 + RES, group * LANE:(group + 1) * LANE], diag(*halves))

    def weighted(pair, group):
        lanes = slice(pair * LANE, (pair + 1) * LANE)
        first, second = probs.pop((pair, group, 0)), probs.pop((pair, group, 1))
        for t in range(2):
            part = slice(t * LANE, (t + 1) * LANE)
            rows = slice(group * LANE + t * RES, group * LANE + (t + 1) * RES)
            both = dot_nn(v[rows, lanes], diag(first[:, part], second[:, part]))
            b0, b1 = both[:, :LANE], both[:, LANE:]
            out = jnp.concatenate([jnp.where(low, b0[:HEAD], pltpu.roll(b1[:HEAD], RES, 1)),
                                   jnp.where(low, pltpu.roll(b0[HEAD:], RES, 1), b1[HEAD:])], axis=0)
            o[rows, lanes] = (out * g[rows, lanes]).astype(BF16)

    units = [(pair, group, s) for pair in range(2) for group in range(groups) for s in range(2)]
    pend = {u: logits(*u) for u in units[:ahead]}
    probs = {}
    for i in range(len(units) + late):
        if i + ahead < len(units):
            pend[units[i + ahead]] = logits(*units[i + ahead])
        if i >= late and units[i - late][2]:
            weighted(*units[i - late][:2])
        if i < len(units):
            pair, group, s = units[i]
            t = pend.pop(units[i]) * SCALE + bias[:, group * SEQ:(group + 1) * SEQ]
            probs[units[i]] = softmax_rows(jnp.where(masks[pair * 2 + s] > 0.5, t, NEG))
        yield


def kernel(n, inputs, *refs):
    hbm, outs, held, sem_in = refs[:inputs], refs[inputs:inputs + 2], refs[inputs + 2:2 * inputs + 2], refs[2 * inputs + 2]
    body(n, hbm, sem_in, outs, *held, *refs[2 * inputs + 3:])


def body(n, hbm, sem_in, outs,
         m_ref, z_ref, mask_ref, res_ref,
         wrb_ref, wri_ref, wro_ref, wci_ref, wco_ref, woi_ref, woo_ref,
         wsb_ref, wsi_ref, wso_ref, web_ref, wei_ref, weo_ref,
         mo, zo, sem_out, mf, zf, mcol, mrow, send_m, send_b, slot_b, bias_r, bias_t, mask_t, mask_n, rnorm, res_col,
           swap, rot, perm_s, perm_r, opm_rhs, opm_stage, opm_send, opm_all, opm_lhs, opm_w, opm_w4, opm_f, opm_t,
           send_z, slot_z,
           cq, ck, cv, cg, co, rq, rk, rv, rg, ro, tq, tk, tv, tg, to,
           ss_b, rs_b, ss_m, rs_m, rs_l, ss_c, rs_c, ss_r, rs_r, ss_z, rs_z):
    held = (m_ref, z_ref, mask_ref, res_ref, wrb_ref, wri_ref, wro_ref, wci_ref, wco_ref, woi_ref, woo_ref,
            wsb_ref, wsi_ref, wso_ref, web_ref, wei_ref, weo_ref)
    loads = [(dst, pltpu.make_async_copy(src, dst, sem_in.at[i])) for i, (src, dst) in enumerate(zip(hbm, held))]
    me = lax.axis_index('dap')
    peers = [lax.rem(me + off, n) for off in range(1, n)]
    partner = me + 1 - 2 * lax.rem(me, 2)
    others = [lax.rem(me + off, n) for off in (2, n - 2, 4)]
    scope = jax.named_scope

    def remote(src, dst, send_sem, recv_sem, peer):
        return pltpu.make_async_remote_copy(src_ref=src, dst_ref=dst, send_sem=send_sem, recv_sem=recv_sem,
                                            device_id={'dap': peer}, device_id_type=pl.DeviceIdType.MESH)

    def load_of(ref):
        return next(c for dst, c in loads if dst is ref)

    def need(*wanted):
        for ref in wanted:
            load_of(ref).wait()

    with scope('barrier'):
        barrier = pltpu.get_barrier_semaphore()
        for peer in peers:
            pl.semaphore_signal(barrier, inc=1, device_id={'dap': peer}, device_id_type=pl.DeviceIdType.MESH)
        order = (z_ref, wrb_ref, mask_ref, m_ref, wri_ref)
        for ref in order + tuple(ref for ref in held if not any(ref is o for o in order)):
            load_of(ref).start()

    def bias_part(idx, w_bias, heads):
        z_cat = jnp.concatenate([layer_norm(zf[l]) for l in range(OWN)], axis=1)
        w = w_bias.astype(F32)
        w_rows = jnp.concatenate([jnp.broadcast_to(w[h:h + 1], (OWN, LANE)) for h in range(heads)], axis=0)
        own = iota(w_rows.shape, 0) % OWN
        lhs = jnp.concatenate([jnp.where(own == l, w_rows, 0.0).astype(BF16) for l in range(OWN)], axis=1)
        part = dot_nt(lhs, jnp.concatenate([z_cat, z_cat], axis=0))
        if heads < OWN:
            part = jnp.concatenate([part, jnp.zeros((RES - part.shape[0], LANE), F32)], axis=0)
        part = part.astype(BF16)
        send_b[idx] = part
        slot_b[idx, me] = part

    def bias_send(idx, w_bias, heads):
        bias_part(idx, w_bias, heads)
        bias_start(idx)

    def bias_start(idx):
        for j, peer in enumerate(peers):
            remote(send_b.at[idx], slot_b.at[idx, me], ss_b.at[idx, j], rs_b.at[idx, me], peer).start()

    def bias_slots(idx):
        with scope('bias_wait'):
            for j, src in enumerate(peers):
                c = remote(send_b.at[idx], slot_b.at[idx, src], ss_b.at[idx, j], rs_b.at[idx, src], src)
                c.wait_send()
                c.wait_recv()
        return jnp.concatenate([slot_b[idx, d] for d in range(n)], axis=0)

    def bias_query_local(idx, heads, out):
        full = dot_tn(bias_slots(idx), swap[:, :heads * RES])
        out[...] = full[:RES] * LOG2E

    def bias_key_local(idx, heads, out):
        full = dot_nn(swap[:heads * RES, :], bias_slots(idx)) * LOG2E
        low = iota((RES, LANE), 1) < RES
        for t in range(heads // 2):
            lanes = slice(t * LANE, (t + 1) * LANE)
            out[:, lanes] = jnp.where(low, full[lanes][:RES], full[lanes][RES:])

    GROUPS = OWN

    def row_bufs(grp, slot):
        return [buf.at[grp] for buf in (rq, rk, rv, rg)] + [ro.at[slot]]

    def row_prepare(b, load):
        ro[2:4] = jnp.zeros((2, SEQ, SEQ), BF16)

        def body(half, carry):
            parts = []
            for j in range(GROUPS // 2):
                grp = half * (GROUPS // 2) + j
                parts.append(project(functools.partial(load, grp), wri_ref.at[b], row_bufs(grp, 0)))
            interleave(*parts)
            return carry
        lax.fori_loop(0, 2, body, 0)

    def row_pass(b, load, store, hook):
        def finish(grp, slot):
            yield
            upd = dot_tn(ro[slot], wro_ref[b])
            yield
            store(grp, rounded(load(grp) + upd).reshape(4, RES, SEQ))
            yield

        def body(step, carry):
            s = lax.rem(step, 2) * 2
            parts = []
            for j in range(2):
                grp = step * 2 + j
                masks = [column(mask_t[...], me * HEAD + grp * 4 + r) for r in range(4)]
                parts.append(row_attend(row_bufs(grp, s + j), bias_r, masks))
                parts.append(finish(jnp.maximum(grp - 2, 0), 2 - s + j))
            interleave(*parts)
            hook(step)
            return carry
        lax.fori_loop(0, GROUPS // 2, body, 0)
        interleave(finish(GROUPS - 2, 2), finish(GROUPS - 1, 3))

    def triangle(idx, w_in, w_out, assemble):
        assemble(idx, 4, bias_t)
        with scope('tri'):
            masks = [res_col[:, 0:1]] * 4
            bufs = [[buf.at[c] for buf in (tq, tk, tv, tg, to)] for c in range(2)]
            load = [lambda c=c: zf[c * 4:(c + 1) * 4].reshape(SEQ, LANE) for c in range(2)]

            def finish(c):
                yield
                upd = dot_tn(to[c], w_out)
                yield
                zf[c * 4:(c + 1) * 4] = rounded(load[c]() + upd).reshape(4, RES, LANE)
            interleave(project(load[0], w_in, bufs[0]), project(load[1], w_in, bufs[1]))
            interleave(row_attend(bufs[0], bias_t, masks), row_attend(bufs[1], bias_t, masks))
            interleave(finish(0), finish(1))

    def z_send(idx):
        out = dot_nn(swap[...], zf[...].reshape(OWN * RES, LANE).astype(BF16)).astype(BF16)
        for d in range(n):
            send_z[idx, d] = out[d * RES:(d + 1) * RES]
        slot_z[idx, me] = send_z[idx, me]
        for j, peer in enumerate(peers):
            remote(send_z.at[idx, peer], slot_z.at[idx, me], ss_z.at[idx, j], rs_z.at[idx, me], peer).start()

    def z_recv(idx):
        with scope('z_wait'):
            for j, peer in enumerate(peers):
                c = remote(send_z.at[idx, peer], slot_z.at[idx, peer], ss_z.at[idx, j], rs_z.at[idx, peer], peer)
                c.wait_send()
                c.wait_recv()
        zf[...] = dot_nn(rot[...], jnp.concatenate([slot_z[idx, d] for d in range(n)], axis=0)).reshape(OWN, RES, LANE)

    def partner_of(dev):
        return dev + 1 - 2 * lax.rem(dev, 2)

    def opm_start(b, half):
        turn = selector(HEAD, HEAD, lambda r: r % 4 * OWN + r // 4)
        out = dot_nn(turn, opm_stage[half * HEAD:(half + 1) * HEAD].astype(BF16)).astype(BF16)
        opm_send[b, half] = out
        opm_all[b, me, half] = out
        for j, peer in enumerate([partner] + others):
            remote(opm_send.at[b, half], opm_all.at[b, me, half], ss_c.at[b, half, j], rs_c.at[b, half, me], peer).start()

    def opm_forward(b, half):
        with scope('opm_fwd'):
            for j, src in enumerate(others):
                slot = opm_all.at[b, src, half]
                c = remote(slot, slot, ss_c.at[b, half, len(others) + 1 + j], rs_c.at[b, half, src], partner)
                c.wait_recv()
                c.start()

    def opm_finish(b, w_out):
        with scope('opm_wait'):
            for half in range(2):
                for src in [partner] + [partner_of(o) for o in others]:
                    slot = opm_all.at[b, src, half]
                    remote(slot, slot, ss_c.at[b, half, 0], rs_c.at[b, half, src], partner).wait_recv()
                for j in range(n - 1):
                    slot = opm_send.at[b, half]
                    remote(slot, slot, ss_c.at[b, half, j], rs_c.at[b, half, me], partner).wait_send()
        with scope('opm'):
            lhs = opm_all[b].reshape(OWN * RES, WIDE)
            first = iota((n * 4, OWN, SEQ), 1) < 4
            for pair in range(OWN // 2):
                part = rounded(dot_nn(lhs, opm_rhs[b, pair])).reshape(n, 2, 4, OWN, SEQ)
                h0, h1 = (part[:, half].reshape(n * 4, OWN, SEQ) for half in range(2))
                turned = (jnp.where(first, h0, pltpu.roll(h1, 4, 1)), jnp.where(first, pltpu.roll(h0, 4, 1), h1))
                for g in range(OWN):
                    rows = turned[g % 2].reshape(n, 4, OWN, SEQ)[:, g // 2].reshape(RES, SEQ)
                    for half in range(2):
                        l = pair * 2 + half
                        opm_lhs[l * RES:(l + 1) * RES, g * LANE:(g + 1) * LANE] = rows[:, half * LANE:(half + 1) * LANE]
            upd = dot_nn(opm_lhs[...].astype(BF16), w_out).reshape(OWN, RES, LANE)
            zf[...] = rounded(zf[...] + upd * rnorm[...])

    flat = OWN * RES
    with scope('bias0'):
        need(z_ref, wrb_ref)
        zf[...] = z_ref[...].astype(F32)
        bias_part(0, wrb_ref[0], OWN)
        swap[...] = selector(flat, flat, lambda r: r // OWN % OWN * RES + r // RES * OWN + r % OWN)
        perm_s[...] = selector(RES, RES, lambda r: r % OWN * OWN + r // OWN)
        pl.semaphore_wait(barrier, n - 1)
        bias_start(0)
        need(mask_ref)
        mask_t[...] = mask_ref[...].astype(F32)

    def constants():
        need(res_ref, woi_ref, woo_ref)
        rot[...] = selector(flat, flat, lambda r: r // OWN % OWN * RES + r % OWN * OWN + r // RES)
        perm_r[...] = selector(SEQ, SEQ, lambda r: r % OWN * HEAD + r // OWN)
        m_t = mask_t[...]
        mask_n[...] = m_t.T
        norm = dot_nt(m_t.astype(BF16), m_t.astype(BF16))
        for l in range(OWN):
            rnorm[l] = jnp.broadcast_to(1.0 / (1e-3 + column(norm, me * OWN + l)), (RES, LANE))
        res = jnp.broadcast_to(res_ref[...].astype(F32), (RES, RES))
        eye = iota(res.shape, 0) == iota(res.shape, 1)
        res_col[...] = jnp.broadcast_to(jnp.sum(jnp.where(eye, res, 0.0), axis=1, keepdims=True), res_col.shape)
        spread = selector(HEAD, HEAD, lambda r: r % OWN * 4 + r // OWN)
        for b in range(2):
            a, c = woi_ref[b, 0:HEAD], woi_ref[b, HEAD:RES]
            gat, loc = (c, a) if b == 0 else (a, c)
            opm_w[b] = dot_nn(spread, gat).astype(BF16)
            opm_w4[b] = jnp.concatenate([loc] * 4, axis=0)
        opm_f[...] = woo_ref[0].astype(F32)
        for r in range(HEAD):
            opm_t[r * HEAD:(r + 1) * HEAD] = opm_f[pl.ds(r, HEAD, stride=HEAD), :].astype(BF16)
        co[1] = jnp.zeros(co.shape[1:], BF16)

    def send_chunk(chunk):
        rows = pl.ds(pl.multiple_of(chunk * OWN, OWN), OWN)
        dests = [me] + peers
        blks = [mf[rows, pl.ds(pl.multiple_of(dst * OWN, OWN), OWN), :].reshape(RES, SEQ).astype(BF16) for dst in dests]
        out = dot_nn(perm_s[...], jnp.concatenate(blks, axis=1))
        mine = me * CHUNKS + chunk
        for j in range(n):
            blk = out[:, j * SEQ:(j + 1) * SEQ].reshape(OWN, OWN, SEQ).astype(BF16)
            if j == 0:
                mcol[0:OWN, mine] = blk
            else:
                send_m[chunk, j - 1] = blk
        for j, peer in enumerate(peers):
            remote(send_m.at[chunk, j, 0:EARLY], mcol.at[0:EARLY, mine], ss_m.at[0], rs_m.at[chunk], peer).start()

    def send_rest():
        for i in range(EARLY, OWN):
            for j, peer in enumerate(peers):
                remote(send_m.at[:, j, i], mcol.at[i, pl.ds(me * CHUNKS, CHUNKS)], ss_m.at[1], rs_l.at[i], peer).start()

    def at(step, when, fn):
        @pl.when(step == when)
        def _():
            fn()

    def load_first(grp):
        return m_ref[pl.ds(grp * 4, 4)].reshape(SEQ, SEQ).astype(F32)

    def store_first(grp, value):
        mf[pl.ds(grp * 4, 4)] = value

    with scope('prep1'):
        need(m_ref, wri_ref)
        row_prepare(0, load_first)
    bias_query_local(0, OWN, bias_r)
    with scope('row1'):
        need(wro_ref)
        def first_hook(step):
            @pl.when(step > 0)
            def _():
                send_chunk(step - 1)
        row_pass(0, load_first, store_first, first_hook)
    with scope('send_chunk'):
        send_chunk(CHUNKS - 1)
        send_rest()
    with scope('consts'):
        constants()

    col_bufs = lambda s: [buf.at[s] for buf in (cq, ck, cv, cg, co)]

    def residue_wait(i):
        slot = send_m.at[:, :, 0]
        pltpu.make_async_copy(slot, slot, rs_l.at[i]).wait()

    def load_col(i):
        return mcol[i].astype(F32).reshape(SEQ, SEQ)

    def col_finish(b, i, slot):
        safe = jnp.minimum(i, OWN - 1)
        yield
        upd = dot_tn(co[slot], wco_ref[b])
        yield
        x = rounded(load_col(i) + upd)
        mcol[i] = x.reshape(HEAD, OWN, SEQ).astype(BF16)
        x = layer_norm(x)
        yield
        local = (dot_nt(x, opm_w4[b]) * column(mask_n[...], me * OWN + safe)).astype(BF16)
        part = iota(local.shape, 1) // HEAD
        lanes = pl.ds(pl.multiple_of(lax.rem(i, 2) * LANE, LANE), LANE)
        for r in range(4):
            opm_rhs[b, lax.div(i, 2), r * SEQ:(r + 1) * SEQ, lanes] = jnp.where(part == r, local, jnp.zeros_like(local))
        yield
        gathered = rounded(dot_nt(opm_w[b], x) * mask_t[pl.ds(me * OWN + safe, 1), :])
        for r in range(4):
            opm_stage[pl.ds(pl.multiple_of(i * OWN, OWN), OWN), r * SEQ:(r + 1) * SEQ] = gathered[r * OWN:(r + 1) * OWN]
        yield

    def send_back(i):
        mrow[me, i] = mcol[i, pl.ds(me * CHUNKS, CHUNKS)]
        for j, peer in enumerate(peers):
            remote(mcol.at[i, pl.ds(peer * CHUNKS, CHUNKS)], mrow.at[me, i], ss_r.at[j], rs_r.at[me], peer).start()

    need(wsb_ref, wsi_ref, wso_ref, web_ref, wei_ref, weo_ref)
    with scope('col_first'):
        need(wci_ref, wco_ref)
        for chunk in range(CHUNKS):
            slot = send_m.at[chunk, :, 0:EARLY]
            pltpu.make_async_copy(slot, slot, rs_m.at[chunk]).wait()
        interleave(project(lambda: load_col(0), wci_ref.at[0], col_bufs(0)))

    def stage_opm():
        opm_forward(0, 1)
        opm_finish(0, opm_t[...])
        bias_send(1, wsb_ref[0], 4)

    def stage_start():
        triangle(1, wsi_ref.at[0], wso_ref[0], bias_query_local)
        z_send(0)
        bias_send(2, web_ref[0], 4)

    def col_body(step, carry):
        @pl.when(jnp.logical_and(step >= EARLY - 1, step < OWN - 1))
        def _():
            residue_wait(step + 1)
        with scope('col'):
            s = lax.rem(step, 2)
            keep = column(mask_n[...], me * OWN + lax.rem(step, OWN)) > 0.5
            nxt, prev = step + 1, step - 1
            interleave(
                col_attend(col_bufs(s), keep),
                project(lambda: load_col(lax.rem(nxt, OWN)), wci_ref.at[jnp.minimum(lax.div(nxt, OWN), 1)], col_bufs(1 - s)),
                col_finish(jnp.where(prev >= OWN, 1, 0), jnp.where(step == 0, OWN, lax.rem(jnp.maximum(prev, 0), OWN)), 1 - s))

        at(step, 4, lambda: opm_start(0, 0))
        at(step, OWN, lambda: opm_start(0, 1))
        at(step, OWN, lambda: opm_forward(0, 0))
        at(step, OWN + 4, stage_opm)
        at(step, OWN + 4, lambda: opm_start(1, 0))
        at(step, OWN + 6, stage_start)

        @pl.when(prev >= OWN)
        def _():
            send_back(prev - OWN)
        return carry
    lax.fori_loop(0, 2 * OWN, col_body, 0)
    with scope('col_last'):
        interleave(col_finish(1, OWN - 1, 1))
        send_back(OWN - 1)
        opm_start(1, 1)

    z_recv(0)
    triangle(2, wei_ref.at[0], weo_ref[0], bias_key_local)

    with scope('bias3'):
        bias_send(3, wrb_ref[1], OWN)
    opm_forward(1, 0)
    with scope('m_wait'):
        for half in range(2):
            sent = send_m.at[:, :, 0:EARLY] if half == 0 else send_m.at[:, :, EARLY:OWN]
            pltpu.make_async_copy(sent, sent, ss_m.at[half]).wait()
        for j, src in enumerate(peers):
            pltpu.make_async_copy(mrow.at[src], mrow.at[src], rs_r.at[src]).wait()
            pltpu.make_async_copy(mrow.at[src], mrow.at[src], ss_r.at[j]).wait()
    with scope('m_perm'):
        for d in range(n):
            mf[:, d * OWN:(d + 1) * OWN, :] = dot_nn(perm_r[...], mrow[d].astype(F32).reshape(SEQ, SEQ).astype(BF16)).reshape(HEAD, OWN, SEQ)

    def load_second(grp):
        return mf[pl.ds(grp * 4, 4)].reshape(SEQ, SEQ)

    def store_second(grp, value):
        mo[pl.ds(grp * 4, 4)] = value.astype(BF16)

    with scope('prep2'):
        row_prepare(1, load_second)
    opm_forward(1, 1)
    opm_finish(1, woo_ref[1])
    with scope('bias4'):
        bias_send(4, web_ref[1], 4)
    bias_key_local(3, OWN, bias_r)

    def stage_end2():
        triangle(4, wei_ref.at[1], weo_ref[1], bias_query_local)
        z_send(1)
        bias_send(5, wsb_ref[1], 4)

    with scope('row2'):
        row_pass(1, load_second, store_second, lambda step: at(step, 2, stage_end2))
    finals = [pltpu.make_async_copy(src, dst, sem_out.at[i]) for i, (src, dst) in enumerate(zip((mo, zo), outs))]
    finals[0].start()
    z_recv(1)
    triangle(5, wsi_ref.at[1], wso_ref[1], bias_key_local)
    zo[...] = zf[...].astype(BF16)
    finals[1].start()
    for copy in finals:
        copy.wait()


def solution(mesh):
    n = mesh.shape['dap']

    def local_step(msa, pair, msa_mask, res_mask, w_row_bias, w_row_in, w_row_out, w_col_in, w_col_out, w_opm_in, w_opm_out, w_ts_bias, w_ts_in, w_ts_out, w_te_bias, w_te_in, w_te_out):
        flat_in = lambda w: jnp.moveaxis(w, 1, -1).reshape(2, -1, w.shape[1])
        flat_out = lambda w: w.reshape(2, -1, w.shape[-1])
        args = (msa, pair, msa_mask.T, res_mask.reshape(1, -1),
                jnp.swapaxes(w_row_bias, 1, 2), flat_in(w_row_in), flat_out(w_row_out),
                flat_in(w_col_in), flat_out(w_col_out), flat_in(w_opm_in), flat_out(w_opm_out),
                jnp.swapaxes(w_ts_bias, 1, 2), flat_in(w_ts_in), flat_out(w_ts_out),
                jnp.swapaxes(w_te_bias, 1, 2), flat_in(w_te_in), flat_out(w_te_out))
        dma = pltpu.SemaphoreType.DMA

        def work_set(slots, width, q_type, outs=2):
            return [VMEM((slots, width, SEQ), q_type), VMEM((slots, SEQ, width), BF16), VMEM((slots, width, SEQ), BF16),
                    VMEM((slots, width, SEQ), F32), VMEM((outs, width, SEQ), BF16)]
        flat = OWN * RES
        return pl.pallas_call(
            functools.partial(kernel, n, len(args)),
            out_shape=(jax.ShapeDtypeStruct(msa.shape, BF16), jax.ShapeDtypeStruct(pair.shape, BF16)),
            in_specs=[pl.BlockSpec(memory_space=pl.ANY)] * len(args),
            out_specs=(pl.BlockSpec(memory_space=pl.ANY), pl.BlockSpec(memory_space=pl.ANY)),
            scratch_shapes=[
                *[VMEM(a.shape, a.dtype) for a in args], dma((len(args),)),
                VMEM(msa.shape, BF16), VMEM(pair.shape, BF16), dma((2,)),
                VMEM((HEAD, RES, SEQ), F32),
                VMEM((OWN, RES, LANE), F32),
                VMEM((OWN + 1, HEAD, OWN, SEQ), BF16),
                VMEM((n, OWN, CHUNKS, OWN, SEQ), BF16),
                VMEM((CHUNKS, n - 1, OWN, OWN, SEQ), BF16),
                VMEM((6, RES, LANE), BF16),
                VMEM((6, n, RES, LANE), BF16),
                VMEM((RES, flat), F32),
                VMEM((RES, SEQ), F32),
                VMEM((RES, SEQ), F32),
                VMEM((SEQ, RES), F32),
                VMEM((OWN, RES, LANE), F32),
                VMEM((RES, LANE), F32),
                VMEM((flat, flat), BF16),
                VMEM((flat, flat), BF16),
                VMEM((RES, RES), BF16),
                VMEM((SEQ, SEQ), BF16),
                VMEM((2, OWN // 2 + 1, WIDE, SEQ), BF16),
                VMEM((RES + OWN, WIDE), F32),
                VMEM((2, 2, HEAD, WIDE), BF16),
                VMEM((2, n, 2, HEAD, WIDE), BF16),
                VMEM((flat, WIDE), F32),
                VMEM((2, HEAD, SEQ), BF16),
                VMEM((2, LANE, SEQ), BF16),
                VMEM((WIDE, LANE), F32),
                VMEM((WIDE, LANE), BF16),
                VMEM((2, n, RES, LANE), BF16),
                VMEM((2, n, RES, LANE), BF16),
                *work_set(2, SEQ, BF16), *work_set(OWN, SEQ, F32, 4), *work_set(2, LANE, F32),
                dma((6, n - 1)), dma((6, n)), dma((2,)), dma((CHUNKS,)), dma((OWN,)), dma((2, 2, n - 1)), dma((2, 2, n)),
                dma((n - 1,)), dma((n,)), dma((2, n - 1)), dma((2, n)),
            ],
            compiler_params=pltpu.CompilerParams(
                collective_id=0, has_side_effects=True, vmem_limit_bytes=60 * WIDE * WIDE),
            name='evoformer',
        )(*args)

    in_specs = (P(('data', 'dap')), P(('data', 'dap')), P('data'), P('data')) + (P(),) * 13
    out_specs = (P(('data', 'dap')), P(('data', 'dap')))
    return jax.shard_map(local_step, mesh=mesh, in_specs=in_specs, out_specs=out_specs, check_vma=False)
```
